256 devices in a mesh: lon: 32 (over x_lo, z, core), lat: 8 (over x_hi, y).
Axes of the slice: x: 4 (x_hi: 2, x_lo: 2; x = x_hi * 2 + x_lo), y: 4, z: 8, core: 2. Of those that a mesh axis runs over, the one named last changes fastest.
Arguments:
- zonal_state: float32 [4, 32, 3, 32, 4096], P(None, None, None, 'lat', 'lon'), may hold values from -6 to 6
- zonal_courant: float32 [32, 32, 4096], P(None, 'lat', 'lon'), may hold values from -0.5 to 0.5
- zonal_length: int32 [32], P('lat'), may hold values from 1024 to 4096, as said below
- zonal_owner: int32 [32, 4096], P('lat', 'lon'), may hold values from 0 to 127, as said below
- merid_state: float32 [4, 32, 3, 128, 1024], P(None, None, None, 'lon', 'lat'), may hold values from -6 to 6
- merid_courant: float32 [32, 128, 1024], P(None, 'lon', 'lat'), may hold values from -0.5 to 0.5
- mixing: float32 [4, 32, 32], replicated, may hold values from -0.18 to 0.18
Outputs:
- zonal_next: float32 [4, 32, 3, 32, 4096], P(None, None, None, 'lat', 'lon')
- merid_next: float32 [4, 32, 3, 128, 1024], P(None, None, None, 'lon', 'lat')
- coupling: float32 [128, 32, 128], P('lon', 'lat')
The draws below stay inside these ranges and needn't reach their ends.
Inputs may be any that keep to these rules, and one draw needn't show every extreme that they name: `zonal_owner`: non-decreasing along each row; each GCM column holds 16 to 48 consecutive cells of a row, and cell x belongs to a column g with |g - x // 32| <= 1. `zonal_length`: in each latitude sector (aligned blocks of 4 cycles) the first cycle holds 2112 cells and the second 4096.
All inputs are finite; a program needn't handle non-finite values.
Results may differ from the reference program's by a relative error of at most 0.0003.
Values sent between devices are 32-bit elements; how exact they have to be, the bound alone decides.
A program may use at most 64 MiB of HBM per device.

```python
import jax
import jax.numpy as jnp
from jax import lax

NV = 4
LEV = 32
WID = 3
SUB = 4
ZROWS_DEV = 4
CELLS_DEV = 128
GLON_DEV = 4
ZROWS = 32
ZCELLS = 4096
GLON = 128
MCOLS = 128
MY = 1024


def draw_zonal_length(key, part):
    lengths = jax.random.randint(jax.random.fold_in(key, 5), (ZROWS,), ZCELLS // 4, ZCELLS + 1).astype(jnp.int32)
    rows = jnp.arange(ZROWS, dtype=jnp.int32)
    opposite = ZCELLS // 2 + CELLS_DEV // 2
    lengths = jnp.where(rows % ZROWS_DEV == 0, opposite, lengths)
    lengths = jnp.where(rows % ZROWS_DEV == 1, ZCELLS, lengths)
    return lengths.astype(jnp.int32)


def draw_zonal_owner(key, part):
    share = CELLS_DEV // GLON_DEV
    half = share // 2
    pairs = (GLON - 2) // 2
    shifts = jax.random.randint(jax.random.fold_in(key, 11), (ZROWS, pairs), -half, half + 1).astype(jnp.int32)
    shifts = shifts.at[0, 0].set(half)
    inner = jnp.stack([share + shifts, share - shifts], axis=-1).reshape(ZROWS, 2 * pairs)
    edge = jnp.full((ZROWS, 1), share, dtype=jnp.int32)
    widths = jnp.concatenate([edge, inner, edge], axis=1)
    ends = jnp.cumsum(widths, axis=1).astype(jnp.int32)
    cells = jnp.arange(ZCELLS, dtype=jnp.int32)

    def one_row(row_ends):
        return jnp.searchsorted(row_ends, cells, side='right').astype(jnp.int32)
    return jax.vmap(one_row)(ends).astype(jnp.int32)


def steps_of(own_key, shape, pieces, low, high):
    def one(axis_at, blocks):
        steps = jax.random.uniform(jax.random.fold_in(jax.random.fold_in(own_key, 6), axis_at), (blocks,), jnp.float32, low / len(pieces), high / len(pieces))
        return jnp.repeat(jnp.exp(steps), shape[axis_at] // blocks).reshape((-1,) + (1,) * (len(shape) - axis_at - 1))

    factor_of = one(*pieces[0])
    for cut in pieces[1:]:
        factor_of = factor_of * one(*cut)
    return factor_of


def normal_values(key, shape, deviation, bound, pieces=(), kind=jnp.bfloat16):
    entries = deviation * jax.random.normal(key, shape, jnp.float32)
    if pieces:
        entries = entries * steps_of(key, shape, pieces, -0.22, 0.18)
    return jnp.clip(entries, -bound, bound).astype(kind)


def setup_inputs(seed: int = 0) -> dict:
    key_of = jax.random.split(jax.random.key(seed), 8)
    zonal_state = normal_values(key_of[0], (NV, LEV, WID, ZROWS, ZCELLS), 1.0, 6.0, ((3, 8), (4, 32)), jnp.float32)
    zonal_courant = jnp.clip(jax.random.uniform(key_of[1], (LEV, ZROWS, ZCELLS), jnp.float32, -0.5, 0.5) * steps_of(key_of[1], (LEV, ZROWS, ZCELLS), ((1, 8), (2, 32)), -0.4, 0.0), -0.5, 0.5)
    zonal_length = draw_zonal_length(jax.random.fold_in(key_of[7], 71), 0)
    zonal_owner = draw_zonal_owner(jax.random.fold_in(key_of[7], 71), 0)
    merid_state = normal_values(key_of[4], (NV, LEV, WID, MCOLS, MY), 1.0, 6.0, ((3, 32), (4, 8)), jnp.float32)
    merid_courant = jnp.clip(jax.random.uniform(key_of[5], (LEV, MCOLS, MY), jnp.float32, -0.5, 0.5) * steps_of(key_of[5], (LEV, MCOLS, MY), ((1, 32), (2, 8)), -0.4, 0.0), -0.5, 0.5)
    mixing = normal_values(key_of[6], (NV, LEV, LEV), 0.03, 0.18, (), jnp.float32)
    return dict(zonal_state=zonal_state, zonal_courant=zonal_courant, zonal_length=zonal_length, zonal_owner=zonal_owner, merid_state=merid_state, merid_courant=merid_courant, mixing=mixing)


diffuse_along = 0.3
diffuse_across = 0.1


def across_terms(field_now):
    plus_side = jnp.concatenate([field_now[:, :, 1:], field_now[:, :, 2:3]], axis=2)
    minus_side = jnp.concatenate([field_now[:, :, 0:1], field_now[:, :, :2]], axis=2)
    return diffuse_across * (plus_side + minus_side - 2.0 * field_now)


def tendency(field_now, forward_side, backward_side, courant, mixing):
    vertical = jnp.einsum("vkj,vjwrx->vkwrx", mixing, field_now, precision=lax.Precision.HIGHEST)
    advect = -0.5 * courant * (forward_side - backward_side)
    spread = diffuse_along * (forward_side - 2.0 * field_now + backward_side)
    return advect + spread + across_terms(field_now) + vertical


def reference(zonal_state, zonal_courant, zonal_length, zonal_owner, merid_state, merid_courant, mixing):
    cells = jnp.arange(ZCELLS, dtype=jnp.int32)
    at_tail = cells[None, :] == (zonal_length[:, None] - 1)
    at_head = cells[None, :] == 0
    active = cells[None, :] < zonal_length[:, None]
    zonal_now = zonal_state
    for substep in range(SUB):
        head_cell = zonal_now[..., 0:1]
        tail_cell = jnp.sum(jnp.where(at_tail, zonal_now, 0.0), axis=-1, keepdims=True)
        forward_side = jnp.where(at_tail, head_cell, jnp.roll(zonal_now, -1, axis=-1))
        backward_side = jnp.where(at_head, tail_cell, jnp.roll(zonal_now, 1, axis=-1))
        change = tendency(zonal_now, forward_side, backward_side, zonal_courant[:, None], mixing)
        zonal_now = jnp.where(active, zonal_now + change, zonal_now)
    merid_now = merid_state
    half_turn = MCOLS // 2
    for substep in range(SUB):
        north_edge = jnp.roll(merid_now[:, :, ::-1, :, -1:], -half_turn, axis=3)
        south_edge = jnp.roll(merid_now[:, :, ::-1, :, 0:1], -half_turn, axis=3)
        forward_side = jnp.concatenate([merid_now[..., 1:], north_edge], axis=-1)
        backward_side = jnp.concatenate([south_edge, merid_now[..., :-1]], axis=-1)
        merid_now = merid_now + tendency(merid_now, forward_side, backward_side, merid_courant[:, None], mixing)
    scale = GLON_DEV / (3.0 * CELLS_DEV)
    change_sum = jnp.sum(zonal_now - zonal_state, axis=2) * scale
    flat = change_sum.reshape(NV * LEV, ZROWS, ZCELLS)
    columns = jnp.arange(GLON, dtype=jnp.int32)

    def one_row(paired):
        owner_row, change_row = paired
        onehot = (owner_row[:, None] == columns[None, :]).astype(jnp.float32)
        return jnp.einsum("xg,jx->gj", onehot, change_row, precision=lax.Precision.HIGHEST)

    rows_out = lax.map(one_row, (zonal_owner, jnp.moveaxis(flat, 1, 0)))
    coupling = jnp.transpose(rows_out, (1, 0, 2))
    return zonal_now, merid_now, coupling
```

```python
import functools

import jax
import jax.numpy as jnp
from jax import lax
from jax.experimental import pallas as pl
from jax.experimental.pallas import tpu as pltpu
from jax.sharding import PartitionSpec as P

SUB = 4
OFF = 8
CELLS = 128
LANES = 128
ROWS = 152
WIN = 16
SROWS = 32
PROWS = 272
PBASE = 136
GLON_DEV = 4
FAR = (0, 2, 3)
MESH = pl.DeviceIdType.MESH
F32 = jnp.float32
BF16 = jnp.bfloat16


def two_parts(value):
    high = value.astype(BF16)
    low = (value - high.astype(F32)).astype(BF16)
    return high, low


def advance(src, dst, courant, weights, lhs, products, items, rows, chunk, ahead):
    for n, item in enumerate(items):
        for w in range(3):
            for at in range(0, rows, chunk):
                high, low = two_parts(src(item, w, OFF + at, chunk))
                spot = pl.ds((n * 3 + w) * rows + at, chunk)
                lhs[spot, 0:LANES] = high
                lhs[spot, LANES:] = low
    total = len(items) * 3 * rows
    for at in range(0, total, ahead):
        size = min(ahead, total - at)
        products[pl.ds(at, size), :] = jnp.dot(
            lhs[pl.ds(at, size), :], weights[...], preferred_element_type=F32
        )
    for n, item in enumerate(items):
        for at in range(0, rows, chunk):
            half = 0.5 * courant(item, at, chunk)
            ahead_share, behind_share = 0.3 - half, 0.3 + half
            now = [src(item, w, OFF + at, chunk) for w in range(3)]
            for w, (one, other) in enumerate(((0, 1), (0, 2), (1, 2))):
                spot = pl.ds((n * 3 + w) * rows + at, chunk)
                mixed = products[spot, 0:LANES] + products[spot, LANES:]
                along = ahead_share * src(item, w, OFF + at + 1, chunk) + behind_share * src(
                    item, w, OFF + at - 1, chunk
                )
                dst(item, w, OFF + at, chunk, mixed + along + 0.1 * (now[one] + now[other]))


def kernel(
    counts,
    zlen,
    zs,
    zc,
    owner,
    ms,
    mc,
    mix,
    out_z,
    out_m,
    out_c,
    raw,
    rawc,
    first,
    state,
    weights,
    lhs,
    products,
    strips,
    scour,
    slhs,
    sproducts,
    back,
    edges,
    halos,
    tails,
    gathered,
    gathered_0,
    heads,
    part,
    part_in,
    load_sem,
    send_sem,
    recv_sem,
    far_send,
    far_recv,
):
    lon_count, lat_count = counts
    half_turn = lon_count // 2
    tail_from = lon_count // 4 - 1
    tail_devs = list(range(tail_from, lon_count))
    me, lat = lax.axis_index("lon"), lax.axis_index("lat")
    left = lax.rem(me + lon_count - 1, lon_count)
    right = lax.rem(me + 1, lon_count)
    across = lax.rem(me + half_turn, lon_count)
    at_south, at_north = lat == 0, lat == lat_count - 1
    south = {"lon": jnp.where(at_south, across, me), "lat": jnp.where(at_south, lat, lat - 1)}
    north = {"lon": jnp.where(at_north, across, me), "lat": jnp.where(at_north, lat, lat + 1)}
    west, east = {"lon": left, "lat": lat}, {"lon": right, "lat": lat}
    root = {"lon": 0 * me, "lat": lat}
    is_root, is_tail, is_half = me == 0, me >= tail_from, me == half_turn

    barrier = pltpu.get_barrier_semaphore()
    for peer in (west, east, south, north):
        pl.semaphore_signal(barrier, inc=1, device_id=peer, device_id_type=MESH)

    @pl.when(is_tail)
    def _():
        pl.semaphore_signal(barrier, inc=1, device_id=root, device_id_type=MESH)

    @pl.when(is_root)
    def _():
        for dev in tail_devs:
            pl.semaphore_signal(
                barrier, inc=1, device_id={"lon": 0 * me + dev, "lat": lat}, device_id_type=MESH
            )

    loads = []
    for f, (s_ref, c_ref) in enumerate(((zs, zc), (ms, mc))):
        loads.append(pltpu.make_async_copy(s_ref, raw.at[f], load_sem.at[f, 0]))
        loads.append(pltpu.make_async_copy(c_ref, rawc.at[f], load_sem.at[f, 1]))
    for load in loads:
        load.start()

    spread = jnp.concatenate([mix[...]] * 4, axis=1)
    row_at = lax.broadcasted_iota(jnp.int32, (LANES, LANES), 0)
    lane_at = lax.broadcasted_iota(jnp.int32, (LANES, LANES), 1)
    spread = jnp.where(row_at // 32 == lane_at // 32, spread, 0.0)
    spread = spread + jnp.where(row_at == lane_at, 0.2, 0.0)
    high, low = two_parts(spread.T)
    for row in (0, LANES):
        weights[row : row + LANES, 0:LANES] = high
        weights[row : row + LANES, LANES:] = low

    def turn_in(f):
        loads[2 * f].wait()
        loads[2 * f + 1].wait()
        for r in range(4):
            for w in range(3):
                turned = raw[f, pl.ds(w * 4 + r, LANES, stride=12), :].T
                first[4 * f + r, w, OFF : OFF + CELLS, :] = turned
                state[0, 4 * f + r, w, OFF : OFF + CELLS, :] = turned
            c_now = rawc[f, pl.ds(r, 32, stride=4), :]
            first[4 * f + r, 3, OFF : OFF + CELLS, :] = jnp.concatenate([c_now] * 4, axis=0).T
        for r in range(4):
            for p in range(4):
                edges[f, 0, r, 4 * p : 4 * p + 4, :] = first[4 * f + r, p, OFF : OFF + SUB, :]
                edges[f, 1, r, 4 * p : 4 * p + 4, :] = first[
                    4 * f + r, p, OFF + CELLS - SUB : OFF + CELLS, :
                ]

    turn_in(0)
    ends = [jnp.clip(zlen[r] - me * CELLS, 0, CELLS + SUB) for r in range(4)]
    quarter = lax.broadcasted_iota(jnp.int32, (8, LANES), 0)
    for r in FAR:
        cell = ends[r] - SUB + quarter
        own = (cell >= 0) & (cell < CELLS)
        for p in range(4):
            found = jnp.where(own, first[r, p, pl.ds(OFF + ends[r] - SUB, 8), :], 0.0)
            tails[r, 4 * p : 4 * p + 4, :] = found[0:SUB]
    turn_in(1)

    def interior(f):
        def step(t, carry):
            now, then = lax.rem(t, 2), lax.rem(t + 1, 2)

            def src(ch, w, at, size):
                return state[now, ch, w, pl.ds(at, size), :]

            def dst(ch, w, at, size, value):
                state[then, ch, w, pl.ds(at, size), :] = value

            advance(
                src,
                dst,
                lambda ch, at, size: first[ch, 3, pl.ds(OFF + at, size), :],
                weights,
                lhs,
                products,
                [4 * f + r for r in range(4)],
                CELLS,
                32,
                384,
            )
            return carry

        lax.fori_loop(0, SUB, step, 0)

    interior(0)

    peers = 4 + jnp.where(is_tail, 1, 0) + jnp.where(is_root, len(tail_devs), 0)
    pl.semaphore_wait(barrier, peers)

    def remote(src, dst, s_sem, r_sem, peer):
        return pltpu.make_async_remote_copy(
            src_ref=src,
            dst_ref=dst,
            send_sem=s_sem,
            recv_sem=r_sem,
            device_id=peer,
            device_id_type=MESH,
        )

    slot = jnp.maximum(me - tail_from, 0)
    tail_copy = remote(
        tails.at[2:4], gathered.at[slot], far_send.at[0], far_recv.at[slot], root
    )
    tail_0_copy = remote(
        tails.at[0], gathered_0, far_send.at[1], recv_sem.at[7], root
    )
    head_copies = [
        remote(
            edges.at[0, 0, 2:4],
            heads.at[2:4],
            far_send.at[2 + n],
            recv_sem.at[8],
            {"lon": 0 * me + dev, "lat": lat},
        )
        for n, dev in enumerate(tail_devs)
    ]
    head_0_copy = remote(
        edges.at[0, 0, 0],
        heads.at[0],
        far_send.at[2 + len(tail_devs)],
        recv_sem.at[9],
        {"lon": 0 * me + half_turn, "lat": lat},
    )

    @pl.when(is_tail)
    def _():
        tail_copy.start()

    @pl.when(is_half)
    def _():
        tail_0_copy.start()

    @pl.when(is_root)
    def _():
        head_0_copy.start()
        for copy in head_copies:
            copy.start()

    south_side, north_side = jnp.where(at_south, 0, 1), jnp.where(at_north, 1, 0)
    near = [
        remote(edges.at[0, 0], halos.at[0, 1], send_sem.at[0], recv_sem.at[1], west),
        remote(edges.at[0, 1], halos.at[0, 0], send_sem.at[1], recv_sem.at[0], east),
        remote(
            edges.at[1, 0],
            halos.at[1, south_side],
            send_sem.at[2],
            recv_sem.at[2 + south_side],
            south,
        ),
        remote(
            edges.at[1, 1],
            halos.at[1, north_side],
            send_sem.at[3],
            recv_sem.at[2 + north_side],
            north,
        ),
    ]
    for copy in near:
        copy.start()

    interior(1)

    def arrived(f, side):
        pltpu.make_async_copy(
            halos.at[f, side], halos.at[f, side], recv_sem.at[2 * f + side]
        ).wait()

    def strip_src(now):
        return lambda n, w, at, size: strips[now, n, w, pl.ds(at, size), :]

    def strip_steps(count):
        def step(t, carry):
            now, then = lax.rem(t, 2), lax.rem(t + 1, 2)

            def dst(n, w, at, size, value):
                strips[then, n, w, pl.ds(at, size), :] = value

            advance(
                strip_src(now),
                dst,
                lambda n, at, size: scour[n, pl.ds(at, size), :],
                weights,
                slhs,
                sproducts,
                list(range(count)),
                WIN,
                16,
                count * 3 * WIN,
            )
            return carry

        lax.fori_loop(0, SUB, step, 0)

    def fill(n, ch, start):
        for w in range(3):
            strips[0, n, w, OFF : OFF + WIN, :] = first[ch, w, pl.ds(start, WIN), :]
        scour[n, :, :] = first[ch, 3, pl.ds(start, WIN), :]

    left_row, right_row = OFF - SUB, OFF + CELLS
    for f, side in ((0, 0), (0, 1), (1, 0), (1, 1)):
        arrived(f, side)
    for r in range(4):
        for p in range(4):
            first[r, p, right_row : right_row + SUB, :] = halos[0, 1, r, 4 * p : 4 * p + 4, :]
    for side, turned, row in ((0, at_south, left_row), (1, at_north, right_row)):
        for r in range(4):
            for p in range(4):
                plain = halos[1, side, r, 4 * p : 4 * p + 4, :]
                q = p if p == 3 else 2 - p
                mirrored = jnp.concatenate(
                    [halos[1, side, r, 4 * q + 3 - j : 4 * q + 4 - j, :] for j in range(SUB)],
                    axis=0,
                )
                if p == 3:
                    mirrored = -mirrored
                first[4 + r, p, row : row + SUB, :] = jnp.where(turned, mirrored, plain)
    left_start, right_start = OFF - SUB, OFF + CELLS + SUB - WIN
    for r in range(4):
        fill(r, r, right_start)
        fill(4 + r, 4 + r, left_start)
        fill(8 + r, 4 + r, right_start)
    strip_steps(12)
    for r in range(4):
        for w in range(3):
            kept = strips[0, r, w, OFF + 8 : OFF + 12, :]
            state[0, r, w, OFF + CELLS - SUB : OFF + CELLS, :] = kept
            kept = strips[0, 4 + r, w, OFF + 4 : OFF + 8, :]
            state[0, 4 + r, w, OFF : OFF + SUB, :] = kept
            kept = strips[0, 8 + r, w, OFF + 8 : OFF + 12, :]
            state[0, 4 + r, w, OFF + CELLS - SUB : OFF + CELLS, :] = kept
    for r in range(4):
        for w in range(3):
            out_m[pl.ds(w * 4 + r, LANES, stride=12), :] = state[
                0, 4 + r, w, OFF : OFF + CELLS, :
            ].T

    @pl.when(is_root)
    def _():
        for n in range(len(tail_devs)):
            pltpu.make_async_copy(gathered.at[n], gathered.at[n], far_recv.at[n]).wait()
        pltpu.make_async_copy(gathered_0, gathered_0, recv_sem.at[7]).wait()

    @pl.when(is_tail)
    def _():
        pltpu.make_async_copy(heads.at[2:4], heads.at[2:4], recv_sem.at[8]).wait()

    @pl.when(is_half)
    def _():
        pltpu.make_async_copy(heads.at[0], heads.at[0], recv_sem.at[9]).wait()

    for r in range(4):
        if r == 1:
            tail_cells = None
        elif r == 0:
            tail_cells = gathered_0[...]
        else:
            tail_cells = gathered[0, r - 2]
            for n in range(1, len(tail_devs)):
                tail_cells = tail_cells + gathered[n, r - 2]
        for p in range(4):
            plain = halos[0, 0, r, 4 * p : 4 * p + 4, :]
            if tail_cells is not None:
                plain = jnp.where(is_root, tail_cells[4 * p : 4 * p + 4], plain)
            first[r, p, left_row : left_row + SUB, :] = plain
    for r in range(4):
        fill(r, r, left_start)
    for n, r in enumerate(FAR):
        fill(4 + n, r, ends[r])
        for w in range(3):
            strips[0, 4 + n, w, OFF + 8 : OFF + 12, :] = heads[r, 4 * w : 4 * w + 4, :]
        scour[4 + n, 8:12, :] = heads[r, 12:16, :]
    strip_steps(7)
    for r in range(4):
        for w in range(3):
            kept = strips[0, r, w, OFF + 4 : OFF + 8, :]
            state[0, r, w, OFF : OFF + SUB, :] = kept
    for n, r in enumerate(FAR):
        for w in range(3):
            back[n, w, PBASE : PBASE + WIN, :] = strips[0, 4 + n, w, OFF : OFF + WIN, :]

    near_columns = me * GLON_DEV - 1 + lax.broadcasted_iota(jnp.int32, (8, CELLS), 0)
    column = lax.broadcasted_iota(jnp.int32, (CELLS, LANES), 0)
    scale = GLON_DEV / (3.0 * CELLS)
    for r in range(4):
        change = None
        for w in range(3):
            value = state[0, r, w, OFF : OFF + CELLS, :]
            before = first[r, w, OFF : OFF + CELLS, :]
            if r in FAR:
                n = FAR.index(r)
                cut = ends[r]
                strip = back[n, w, pl.ds(PBASE + 8 - cut, CELLS), :]
                value = jnp.where(column >= cut - SUB, strip, value)
                value = jnp.where(column < cut, value, before)
            out_z[pl.ds(w * 4 + r, LANES, stride=12), :] = value.T
            change = value - before if change is None else change + (value - before)
        high, low = two_parts(change * scale)
        mine = (jnp.broadcast_to(owner[r : r + 1, :], (8, CELLS)) == near_columns).astype(BF16)
        part[r, :, :] = jnp.dot(
            jnp.concatenate([mine, mine], axis=1),
            jnp.concatenate([high, low], axis=0),
            preferred_element_type=F32,
        )
    for r in range(4):
        part[4, r : r + 1, :] = part[r, 0:1, :]
        part[5, r : r + 1, :] = part[r, 5:6, :]
    back_copy = remote(part.at[4], part_in.at[1], send_sem.at[4], recv_sem.at[5], west)
    on_copy = remote(part.at[5], part_in.at[0], send_sem.at[5], recv_sem.at[4], east)
    back_copy.start()
    on_copy.start()
    back_copy.wait_recv()
    on_copy.wait_recv()
    for r in range(4):
        for g in range(GLON_DEV):
            value = part[r, g + 1 : g + 2, :]
            if g == 0:
                value = value + part_in[0, r : r + 1, :]
            if g == GLON_DEV - 1:
                value = value + part_in[1, r : r + 1, :]
            out_c[4 * g + r : 4 * g + r + 1, :] = value

    for copy in near:
        copy.wait_send()
    back_copy.wait_send()
    on_copy.wait_send()

    @pl.when(is_tail)
    def _():
        tail_copy.wait_send()

    @pl.when(is_half)
    def _():
        tail_0_copy.wait_send()

    @pl.when(is_root)
    def _():
        head_0_copy.wait_send()
        for copy in head_copies:
            copy.wait_send()


def shards(
    counts, zonal_state, zonal_courant, zonal_length, zonal_owner, merid_state, merid_courant, mixing
):
    tail_count = counts[0] - (counts[0] // 4 - 1)
    hbm = pl.BlockSpec(memory_space=pltpu.HBM)
    vmem = pl.BlockSpec(memory_space=pltpu.VMEM)
    smem = pl.BlockSpec(memory_space=pltpu.SMEM)
    flat_shape = (LANES * 12, CELLS)
    out_z, out_m, out_c = pl.pallas_call(
        functools.partial(kernel, counts),
        out_shape=(
            jax.ShapeDtypeStruct(flat_shape, F32),
            jax.ShapeDtypeStruct(flat_shape, F32),
            jax.ShapeDtypeStruct((4 * GLON_DEV, LANES), F32),
        ),
        in_specs=[smem, hbm, hbm, vmem, hbm, hbm, vmem],
        out_specs=(vmem, vmem, vmem),
        scratch_shapes=[
            pltpu.VMEM((2, *flat_shape), F32),
            pltpu.VMEM((2, LANES, CELLS), F32),
            pltpu.VMEM((8, 4, ROWS, LANES), F32),
            pltpu.VMEM((2, 8, 3, ROWS, LANES), F32),
            pltpu.VMEM((2 * LANES, 2 * LANES), BF16),
            pltpu.VMEM((4 * 3 * CELLS, 2 * LANES), BF16),
            pltpu.VMEM((4 * 3 * CELLS, 2 * LANES), F32),
            pltpu.VMEM((2, 12, 3, SROWS, LANES), F32),
            pltpu.VMEM((12, WIN, LANES), F32),
            pltpu.VMEM((12 * 3 * WIN, 2 * LANES), BF16),
            pltpu.VMEM((12 * 3 * WIN, 2 * LANES), F32),
            pltpu.VMEM((3, 3, PROWS, LANES), F32),
            pltpu.VMEM((2, 2, 4, 16, LANES), F32),
            pltpu.VMEM((2, 2, 4, 16, LANES), F32),
            pltpu.VMEM((4, 16, LANES), F32),
            pltpu.VMEM((tail_count, 2, 16, LANES), F32),
            pltpu.VMEM((16, LANES), F32),
            pltpu.VMEM((4, 16, LANES), F32),
            pltpu.VMEM((6, 8, LANES), F32),
            pltpu.VMEM((2, 8, LANES), F32),
            pltpu.SemaphoreType.DMA((2, 2)),
            pltpu.SemaphoreType.DMA((6,)),
            pltpu.SemaphoreType.DMA((10,)),
            pltpu.SemaphoreType.DMA((3 + tail_count,)),
            pltpu.SemaphoreType.DMA((tail_count,)),
        ],
        compiler_params=pltpu.CompilerParams(
            collective_id=0, has_side_effects=True, vmem_limit_bytes=32 * 1024 * 1024
        ),
    )(
        zonal_length,
        zonal_state.reshape(flat_shape),
        zonal_courant.reshape(LANES, CELLS),
        zonal_owner,
        merid_state.reshape(flat_shape),
        merid_courant.reshape(LANES, CELLS),
        mixing.reshape(LANES, 32),
    )
    return (
        out_z.reshape(zonal_state.shape),
        out_m.reshape(merid_state.shape),
        out_c.reshape(GLON_DEV, 4, LANES),
    )


def solution(mesh):
    counts = (mesh.shape["lon"], mesh.shape["lat"])
    return jax.shard_map(
        functools.partial(shards, counts),
        mesh=mesh,
        in_specs=(
            P(None, None, None, "lat", "lon"),
            P(None, "lat", "lon"),
            P("lat"),
            P("lat", "lon"),
            P(None, None, None, "lon", "lat"),
            P(None, "lon", "lat"),
            P(),
        ),
        out_specs=(
            P(None, None, None, "lat", "lon"),
            P(None, None, None, "lon", "lat"),
            P("lon", "lat", None),
        ),
        check_vma=False,
    )
```

```python
import functools

import jax
import jax.numpy as jnp
from jax import lax
from jax.experimental import pallas as pl
from jax.experimental.pallas import tpu as pltpu
from jax.sharding import PartitionSpec as P

SUB = 4
OFF = 8
CELLS = 128
LANES = 128
ROWS = 152
WIN = 16
SROWS = 32
PROWS = 272
PBASE = 136
GLON_DEV = 4
FAR = (0, 2, 3)
MESH = pl.DeviceIdType.MESH
F32 = jnp.float32
BF16 = jnp.bfloat16


def two_parts(value):
    high = value.astype(BF16)
    low = (value - high.astype(F32)).astype(BF16)
    return high, low


def advance(src, dst, courant, weights, lhs, products, items, rows, chunk, ahead):
    for n, item in enumerate(items):
        for w in range(3):
            for at in range(0, rows, chunk):
                high, low = two_parts(src(item, w, OFF + at, chunk))
                spot = pl.ds((n * 3 + w) * rows + at, chunk)
                lhs[spot, 0:LANES] = high
                lhs[spot, LANES:] = low
    total = len(items) * 3 * rows
    for at in range(0, total, ahead):
        size = min(ahead, total - at)
        products[pl.ds(at, size), :] = jnp.dot(
            lhs[pl.ds(at, size), :], weights[...], preferred_element_type=F32
        )
    for n, item in enumerate(items):
        for at in range(0, rows, chunk):
            half = 0.5 * courant(item, at, chunk)
            ahead_share, behind_share = 0.3 - half, 0.3 + half
            now = [src(item, w, OFF + at, chunk) for w in range(3)]
            for w, (one, other) in enumerate(((0, 1), (0, 2), (1, 2))):
                spot = pl.ds((n * 3 + w) * rows + at, chunk)
                mixed = products[spot, 0:LANES] + products[spot, LANES:]
                along = ahead_share * src(item, w, OFF + at + 1, chunk) + behind_share * src(
                    item, w, OFF + at - 1, chunk
                )
                dst(item, w, OFF + at, chunk, mixed + along + 0.1 * (now[one] + now[other]))


def kernel(
    counts,
    zlen_ref,
    zs,
    zc,
    owner_ref,
    ms,
    mc,
    mix_ref,
    out_z,
    out_m,
    out_c,
    raw,
    rawc,
    owner,
    mix,
    zlen,
    first,
    state,
    weights,
    lhs,
    products,
    strips,
    scour,
    slhs,
    sproducts,
    back,
    edges,
    halos,
    tails,
    gathered,
    gathered_0,
    heads,
    part,
    part_in,
    load_sem,
    send_sem,
    recv_sem,
    far_send,
    far_recv,
):
    lon_count, lat_count = counts
    half_turn = lon_count // 2
    tail_from = lon_count // 4 - 1
    tail_devs = list(range(tail_from, lon_count))
    me, lat = lax.axis_index("lon"), lax.axis_index("lat")
    left = lax.rem(me + lon_count - 1, lon_count)
    right = lax.rem(me + 1, lon_count)
    across = lax.rem(me + half_turn, lon_count)
    at_south, at_north = lat == 0, lat == lat_count - 1
    south = {"lon": jnp.where(at_south, across, me), "lat": jnp.where(at_south, lat, lat - 1)}
    north = {"lon": jnp.where(at_north, across, me), "lat": jnp.where(at_north, lat, lat + 1)}
    west, east = {"lon": left, "lat": lat}, {"lon": right, "lat": lat}
    root = {"lon": 0 * me, "lat": lat}
    is_root, is_tail, is_half = me == 0, me >= tail_from, me == half_turn

    barrier = pltpu.get_barrier_semaphore()
    for peer in (west, east, south, north):
        pl.semaphore_signal(barrier, inc=1, device_id=peer, device_id_type=MESH)

    @pl.when(is_tail)
    def _():
        pl.semaphore_signal(barrier, inc=1, device_id=root, device_id_type=MESH)

    @pl.when(is_root)
    def _():
        for dev in tail_devs:
            pl.semaphore_signal(
                barrier, inc=1, device_id={"lon": 0 * me + dev, "lat": lat}, device_id_type=MESH
            )

    loads = []
    for f, (s_ref, c_ref) in enumerate(((zs, zc), (ms, mc))):
        loads.append(pltpu.make_async_copy(s_ref, raw.at[f], load_sem.at[f, 0]))
        loads.append(pltpu.make_async_copy(c_ref, rawc.at[f], load_sem.at[f, 1]))
    loads.append(pltpu.make_async_copy(mix_ref, mix, load_sem.at[2, 0]))
    loads.append(pltpu.make_async_copy(owner_ref, owner, load_sem.at[2, 1]))
    loads.append(pltpu.make_async_copy(zlen_ref, zlen, load_sem.at[3, 0]))
    for load in loads:
        load.start()

    def turn_in(f, channels):
        if channels[0] != 1:
            loads[2 * f].wait()
            loads[2 * f + 1].wait()
        for r in channels:
            for w in range(3):
                turned = raw[f, pl.ds(w * 4 + r, LANES, stride=12), :].T
                first[4 * f + r, w, OFF : OFF + CELLS, :] = turned
                state[0, 4 * f + r, w, OFF : OFF + CELLS, :] = turned
            c_now = rawc[f, pl.ds(r, 32, stride=4), :]
            first[4 * f + r, 3, OFF : OFF + CELLS, :] = jnp.concatenate([c_now] * 4, axis=0).T
        for r in channels:
            for p in range(4):
                edges[f, 0, r, 4 * p : 4 * p + 4, :] = first[4 * f + r, p, OFF : OFF + SUB, :]
                edges[f, 1, r, 4 * p : 4 * p + 4, :] = first[
                    4 * f + r, p, OFF + CELLS - SUB : OFF + CELLS, :
                ]

    with jax.named_scope("turn_z"):
        turn_in(0, (2, 3, 0))
        loads[6].wait()
        ends = [jnp.clip(zlen[r] - me * CELLS, 0, CELLS + SUB) for r in range(4)]
        quarter = lax.broadcasted_iota(jnp.int32, (8, LANES), 0)
        for r in FAR:
            cell = ends[r] - SUB + quarter
            own = (cell >= 0) & (cell < CELLS)
            for p in range(4):
                found = jnp.where(own, first[r, p, pl.ds(OFF + ends[r] - SUB, 8), :], 0.0)
                tails[r, 4 * p : 4 * p + 4, :] = found[0:SUB]
        turn_in(0, (1,))

    with jax.named_scope("turn_m"):
        turn_in(1, (0, 1, 2, 3))

    loads[4].wait()
    loads[5].wait()
    spread = jnp.concatenate([mix[...]] * 4, axis=1)
    row_at = lax.broadcasted_iota(jnp.int32, (LANES, LANES), 0)
    lane_at = lax.broadcasted_iota(jnp.int32, (LANES, LANES), 1)
    spread = jnp.where(row_at // 32 == lane_at // 32, spread, 0.0)
    spread = spread + jnp.where(row_at == lane_at, 0.2, 0.0)
    high, low = two_parts(spread.T)
    for row in (0, LANES):
        weights[row : row + LANES, 0:LANES] = high
        weights[row : row + LANES, LANES:] = low


    def interior(f, between=None):
        def step(t, carry):
            if between is not None:
                pl.when(is_root & (t == 2))(between)
            now, then = lax.rem(t, 2), lax.rem(t + 1, 2)

            def src(ch, w, at, size):
                return state[now, ch, w, pl.ds(at, size), :]

            def dst(ch, w, at, size, value):
                state[then, ch, w, pl.ds(at, size), :] = value

            advance(
                src,
                dst,
                lambda ch, at, size: first[ch, 3, pl.ds(OFF + at, size), :],
                weights,
                lhs,
                products,
                [4 * f + r for r in range(4)],
                CELLS,
                32,
                384,
            )
            return carry

        lax.fori_loop(0, SUB, step, 0)

    def remote(src, dst, s_sem, r_sem, peer):
        return pltpu.make_async_remote_copy(
            src_ref=src,
            dst_ref=dst,
            send_sem=s_sem,
            recv_sem=r_sem,
            device_id=peer,
            device_id_type=MESH,
        )

    slot = jnp.maximum(me - tail_from, 0)
    tail_copy = remote(
        tails.at[2:4], gathered.at[slot], far_send.at[0], far_recv.at[slot], root
    )
    tail_0_copy = remote(
        tails.at[0], gathered_0, far_send.at[1], recv_sem.at[7], root
    )
    head_copies = [
        remote(
            edges.at[0, 0, 2:4],
            heads.at[2:4],
            far_send.at[2 + n],
            recv_sem.at[8],
            {"lon": 0 * me + dev, "lat": lat},
        )
        for n, dev in enumerate(tail_devs)
    ]
    head_0_copy = remote(
        edges.at[0, 0, 0],
        heads.at[0],
        far_send.at[2 + len(tail_devs)],
        recv_sem.at[9],
        {"lon": 0 * me + half_turn, "lat": lat},
    )

    south_side, north_side = jnp.where(at_south, 0, 1), jnp.where(at_north, 1, 0)
    near = [
        remote(edges.at[0, 0], halos.at[0, 1], send_sem.at[0], recv_sem.at[1], west),
        remote(edges.at[0, 1], halos.at[0, 0], send_sem.at[1], recv_sem.at[0], east),
        remote(
            edges.at[1, 0],
            halos.at[1, south_side],
            send_sem.at[2],
            recv_sem.at[2 + south_side],
            south,
        ),
        remote(
            edges.at[1, 1],
            halos.at[1, north_side],
            send_sem.at[3],
            recv_sem.at[2 + north_side],
            north,
        ),
    ]
    @pl.when(jnp.logical_not(is_root))
    def _():
        with jax.named_scope("barrier"):
            pl.semaphore_wait(barrier, 4 + jnp.where(is_tail, 1, 0))

        @pl.when(is_tail)
        def _():
            tail_copy.start()

        @pl.when(is_half)
        def _():
            tail_0_copy.start()

        for copy in near:
            copy.start()

    def root_sends():
        with jax.named_scope("barrier_root"):
            pl.semaphore_wait(barrier, 4 + len(tail_devs))
        for copy in near:
            copy.start()
        head_0_copy.start()
        for copy in head_copies:
            copy.start()

    with jax.named_scope("interior_z"):
        interior(0)
    with jax.named_scope("interior_m"):
        interior(1, root_sends)

    def arrived(f, side):
        pltpu.make_async_copy(
            halos.at[f, side], halos.at[f, side], recv_sem.at[2 * f + side]
        ).wait()

    def strip_src(now):
        return lambda n, w, at, size: strips[now, n, w, pl.ds(at, size), :]

    def strip_steps(count):
        def step(t, carry):
            now, then = lax.rem(t, 2), lax.rem(t + 1, 2)

            def dst(n, w, at, size, value):
                strips[then, n, w, pl.ds(at, size), :] = value

            advance(
                strip_src(now),
                dst,
                lambda n, at, size: scour[n, pl.ds(at, size), :],
                weights,
                slhs,
                sproducts,
                list(range(count)),
                WIN,
                16,
                count * 3 * WIN,
            )
            return carry

        lax.fori_loop(0, SUB, step, 0)

    def fill(n, ch, start):
        for w in range(3):
            strips[0, n, w, OFF : OFF + WIN, :] = first[ch, w, pl.ds(start, WIN), :]
        scour[n, :, :] = first[ch, 3, pl.ds(start, WIN), :]

    left_row, right_row = OFF - SUB, OFF + CELLS
    with jax.named_scope("near_wait"):
        for f, side in ((0, 0), (0, 1), (1, 0), (1, 1)):
            arrived(f, side)
    for r in range(4):
        for p in range(4):
            first[r, p, right_row : right_row + SUB, :] = halos[0, 1, r, 4 * p : 4 * p + 4, :]
    for side, turned, row in ((0, at_south, left_row), (1, at_north, right_row)):
        for r in range(4):
            for p in range(4):
                plain = halos[1, side, r, 4 * p : 4 * p + 4, :]
                q = p if p == 3 else 2 - p
                mirrored = jnp.concatenate(
                    [halos[1, side, r, 4 * q + 3 - j : 4 * q + 4 - j, :] for j in range(SUB)],
                    axis=0,
                )
                if p == 3:
                    mirrored = -mirrored
                first[4 + r, p, row : row + SUB, :] = jnp.where(turned, mirrored, plain)
    left_start, right_start = OFF - SUB, OFF + CELLS + SUB - WIN
    for r in range(4):
        fill(r, r, right_start)
        fill(4 + r, 4 + r, left_start)
        fill(8 + r, 4 + r, right_start)
    with jax.named_scope("near_strips"):
        strip_steps(12)
    for r in range(4):
        for w in range(3):
            kept = strips[0, r, w, OFF + 8 : OFF + 12, :]
            state[0, r, w, OFF + CELLS - SUB : OFF + CELLS, :] = kept
            kept = strips[0, 4 + r, w, OFF + 4 : OFF + 8, :]
            state[0, 4 + r, w, OFF : OFF + SUB, :] = kept
            kept = strips[0, 8 + r, w, OFF + 8 : OFF + 12, :]
            state[0, 4 + r, w, OFF + CELLS - SUB : OFF + CELLS, :] = kept
    for r in range(4):
        for w in range(3):
            out_m[pl.ds(w * 4 + r, LANES, stride=12), :] = state[
                0, 4 + r, w, OFF : OFF + CELLS, :
            ].T

    near_columns = me * GLON_DEV - 1 + lax.broadcasted_iota(jnp.int32, (8, CELLS), 0)
    column = lax.broadcasted_iota(jnp.int32, (CELLS, LANES), 0)
    scale = GLON_DEV / (3.0 * CELLS)
    back_copy = remote(part.at[4], part_in.at[1], send_sem.at[4], recv_sem.at[5], west)
    on_copy = remote(part.at[5], part_in.at[0], send_sem.at[5], recv_sem.at[4], east)
    is_last = me == lon_count - 1

    def shares(r, change):
        high, low = two_parts(change * scale)
        mine = (jnp.broadcast_to(owner[r : r + 1, :], (8, CELLS)) == near_columns).astype(BF16)
        return jnp.dot(
            jnp.concatenate([mine, mine], axis=1),
            jnp.concatenate([high, low], axis=0),
            preferred_element_type=F32,
        )

    @pl.when(is_root)
    def _():
        with jax.named_scope("early_part"):
            for r in range(4):
                change = None
                for w in range(3):
                    value = state[0, r, w, OFF : OFF + CELLS, :] - first[r, w, OFF : OFF + CELLS, :]
                    change = value if change is None else change + value
                part[5, r : r + 1, :] = shares(r, change)[5:6]
            on_copy.start()

    with jax.named_scope("far_wait"):
        @pl.when(is_root)
        def _():
            for n in range(len(tail_devs)):
                pltpu.make_async_copy(gathered.at[n], gathered.at[n], far_recv.at[n]).wait()
            pltpu.make_async_copy(gathered_0, gathered_0, recv_sem.at[7]).wait()

        @pl.when(is_tail)
        def _():
            pltpu.make_async_copy(heads.at[2:4], heads.at[2:4], recv_sem.at[8]).wait()

        @pl.when(is_half)
        def _():
            pltpu.make_async_copy(heads.at[0], heads.at[0], recv_sem.at[9]).wait()

    for r in range(4):
        if r == 1:
            tail_cells = None
        elif r == 0:
            tail_cells = gathered_0[...]
        else:
            tail_cells = gathered[0, r - 2]
            for n in range(1, len(tail_devs)):
                tail_cells = tail_cells + gathered[n, r - 2]
        for p in range(4):
            plain = halos[0, 0, r, 4 * p : 4 * p + 4, :]
            if tail_cells is not None:
                plain = jnp.where(is_root, tail_cells[4 * p : 4 * p + 4], plain)
            first[r, p, left_row : left_row + SUB, :] = plain
    for r in range(4):
        fill(r, r, left_start)
    for n, r in enumerate(FAR):
        fill(4 + n, r, ends[r])
        for w in range(3):
            strips[0, 4 + n, w, OFF + 8 : OFF + 12, :] = heads[r, 4 * w : 4 * w + 4, :]
        scour[4 + n, 8:12, :] = heads[r, 12:16, :]
    with jax.named_scope("far_strips"):
        strip_steps(7)
    for r in range(4):
        for w in range(3):
            kept = strips[0, r, w, OFF + 4 : OFF + 8, :]
            state[0, r, w, OFF : OFF + SUB, :] = kept
    for n, r in enumerate(FAR):
        for w in range(3):
            back[n, w, PBASE : PBASE + WIN, :] = strips[0, 4 + n, w, OFF : OFF + WIN, :]

    for r in range(4):
        change = None
        for w in range(3):
            value = state[0, r, w, OFF : OFF + CELLS, :]
            before = first[r, w, OFF : OFF + CELLS, :]
            if r in FAR:
                n = FAR.index(r)
                cut = ends[r]
                strip = back[n, w, pl.ds(PBASE + 8 - cut, CELLS), :]
                value = jnp.where(column >= cut - SUB, strip, value)
                value = jnp.where(column < cut, value, before)
            out_z[pl.ds(w * 4 + r, LANES, stride=12), :] = value.T
            change = value - before if change is None else change + (value - before)
        part[r, :, :] = shares(r, change)

    @pl.when(jnp.logical_not(is_root))
    def _():
        for r in range(4):
            part[4, r : r + 1, :] = part[r, 0:1, :]
        back_copy.start()

    @pl.when(jnp.logical_not(is_root | is_last))
    def _():
        for r in range(4):
            part[5, r : r + 1, :] = part[r, 5:6, :]
        on_copy.start()

    with jax.named_scope("part_wait"):

        @pl.when(is_root)
        def _():
            part_in[0, :, :] = jnp.zeros((8, LANES), F32)

        @pl.when(is_last)
        def _():
            part_in[1, :, :] = jnp.zeros((8, LANES), F32)

        @pl.when(jnp.logical_not(is_last))
        def _():
            back_copy.wait_recv()

        @pl.when(jnp.logical_not(is_root))
        def _():
            on_copy.wait_recv()

    for r in range(4):
        for g in range(GLON_DEV):
            value = part[r, g + 1 : g + 2, :]
            if g == 0:
                value = value + part_in[0, r : r + 1, :]
            if g == GLON_DEV - 1:
                value = value + part_in[1, r : r + 1, :]
            out_c[4 * g + r : 4 * g + r + 1, :] = value

    for copy in near:
        copy.wait_send()

    @pl.when(jnp.logical_not(is_root))
    def _():
        back_copy.wait_send()

    @pl.when(jnp.logical_not(is_last))
    def _():
        on_copy.wait_send()

    @pl.when(is_tail)
    def _():
        tail_copy.wait_send()

    @pl.when(is_half)
    def _():
        tail_0_copy.wait_send()

    @pl.when(is_root)
    def _():
        head_0_copy.wait_send()
        for copy in head_copies:
            copy.wait_send()


def write_out(z, m, c, out_z, out_m, out_c, sem):
    copies = [
        pltpu.make_async_copy(src, dst, sem.at[n])
        for n, (src, dst) in enumerate(((z, out_z), (m, out_m), (c, out_c)))
    ]
    for copy in copies:
        copy.start()
    for copy in copies:
        copy.wait()


def shards(
    counts, zonal_state, zonal_courant, zonal_length, zonal_owner, merid_state, merid_courant, mixing
):
    tail_count = counts[0] - (counts[0] // 4 - 1)
    hbm = pl.BlockSpec(memory_space=pltpu.HBM)
    vmem = pl.BlockSpec(memory_space=pltpu.VMEM)
    flat_shape = (LANES * 12, CELLS)

    def in_hbm(array, shape):
        return pltpu.with_memory_space_constraint(array.reshape(shape), pltpu.HBM)

    out_z, out_m, out_c = pl.pallas_call(
        functools.partial(kernel, counts),
        out_shape=(
            pltpu.VMEM(flat_shape, F32),
            pltpu.VMEM(flat_shape, F32),
            pltpu.VMEM((4 * GLON_DEV, LANES), F32),
        ),
        in_specs=[hbm, hbm, hbm, hbm, hbm, hbm, hbm],
        out_specs=(vmem, vmem, vmem),
        scratch_shapes=[
            pltpu.VMEM((2, *flat_shape), F32),
            pltpu.VMEM((2, LANES, CELLS), F32),
            pltpu.VMEM((4, CELLS), jnp.int32),
            pltpu.VMEM((LANES, 32), F32),
            pltpu.SMEM((4,), jnp.int32),
            pltpu.VMEM((8, 4, ROWS, LANES), F32),
            pltpu.VMEM((2, 8, 3, ROWS, LANES), F32),
            pltpu.VMEM((2 * LANES, 2 * LANES), BF16),
            pltpu.VMEM((4 * 3 * CELLS, 2 * LANES), BF16),
            pltpu.VMEM((4 * 3 * CELLS, 2 * LANES), F32),
            pltpu.VMEM((2, 12, 3, SROWS, LANES), F32),
            pltpu.VMEM((12, WIN, LANES), F32),
            pltpu.VMEM((12 * 3 * WIN, 2 * LANES), BF16),
            pltpu.VMEM((12 * 3 * WIN, 2 * LANES), F32),
            pltpu.VMEM((3, 3, PROWS, LANES), F32),
            pltpu.VMEM((2, 2, 4, 16, LANES), F32),
            pltpu.VMEM((2, 2, 4, 16, LANES), F32),
            pltpu.VMEM((4, 16, LANES), F32),
            pltpu.VMEM((tail_count, 2, 16, LANES), F32),
            pltpu.VMEM((16, LANES), F32),
            pltpu.VMEM((4, 16, LANES), F32),
            pltpu.VMEM((6, 8, LANES), F32),
            pltpu.VMEM((2, 8, LANES), F32),
            pltpu.SemaphoreType.DMA((4, 2)),
            pltpu.SemaphoreType.DMA((6,)),
            pltpu.SemaphoreType.DMA((10,)),
            pltpu.SemaphoreType.DMA((3 + tail_count,)),
            pltpu.SemaphoreType.DMA((tail_count,)),
        ],
        compiler_params=pltpu.CompilerParams(
            collective_id=0, has_side_effects=True, vmem_limit_bytes=32 * 1024 * 1024
        ),
    )(
        in_hbm(zonal_length, (4,)),
        in_hbm(zonal_state, flat_shape),
        in_hbm(zonal_courant, (LANES, CELLS)),
        in_hbm(zonal_owner, (4, CELLS)),
        in_hbm(merid_state, flat_shape),
        in_hbm(merid_courant, (LANES, CELLS)),
        in_hbm(mixing, (LANES, 32)),
    )
    out_z, out_m, out_c = pl.pallas_call(
        write_out,
        out_shape=(
            pltpu.HBM(flat_shape, F32),
            pltpu.HBM(flat_shape, F32),
            pltpu.HBM((4 * GLON_DEV, LANES), F32),
        ),
        in_specs=[vmem, vmem, vmem],
        out_specs=(hbm, hbm, hbm),
        scratch_shapes=[pltpu.SemaphoreType.DMA((3,))],
        compiler_params=pltpu.CompilerParams(vmem_limit_bytes=1024 * 1024),
    )(out_z, out_m, out_c)
    return (
        out_z.reshape(zonal_state.shape),
        out_m.reshape(merid_state.shape),
        out_c.reshape(GLON_DEV, 4, LANES),
    )


def solution(mesh):
    counts = (mesh.shape["lon"], mesh.shape["lat"])
    return jax.shard_map(
        functools.partial(shards, counts),
        mesh=mesh,
        in_specs=(
            P(None, None, None, "lat", "lon"),
            P(None, "lat", "lon"),
            P("lat"),
            P("lat", "lon"),
            P(None, None, None, "lon", "lat"),
            P(None, "lon", "lat"),
            P(),
        ),
        out_specs=(
            P(None, None, None, "lat", "lon"),
            P(None, None, None, "lon", "lat"),
            P("lon", "lat", None),
        ),
        check_vma=False,
    )
```

```python
import functools

import jax
import jax.numpy as jnp
from jax import lax
from jax.experimental import pallas as pl
from jax.experimental.pallas import tpu as pltpu
from jax.sharding import PartitionSpec as P

SUB = 4
OFF = 8
CELLS = 128
LANES = 128
ROWS = 152
WIN = 16
SROWS = 32
PROWS = 272
PBASE = 136
GLON_DEV = 4
FAR = (0, 2, 3)
MESH = pl.DeviceIdType.MESH
F32 = jnp.float32
BF16 = jnp.bfloat16


def two_parts(value):
    high = value.astype(BF16)
    low = (value - high.astype(F32)).astype(BF16)
    return high, low


def advance(src, dst, courant, weights, items, rows, chunk):
    group = max(1, CELLS // rows)
    for first_item in range(0, len(items), group):
        some = items[first_item : first_item + group]
        parts = [
            jnp.concatenate(two_parts(src(item, w, OFF, rows)), axis=1)
            for item in some
            for w in range(3)
        ]
        product = jnp.dot(
            jnp.concatenate(parts, axis=0), weights[...], preferred_element_type=F32
        )
        for n, item in enumerate(some):
            for at in range(0, rows, chunk):
                half = 0.5 * courant(item, at, chunk)
                ahead_share, behind_share = 0.3 - half, 0.3 + half
                here = [src(item, w, OFF + at, chunk) for w in range(3)]
                for w, (one, other) in enumerate(((0, 1), (0, 2), (1, 2))):
                    spot = (n * 3 + w) * rows + at
                    mixed = (
                        product[spot : spot + chunk, 0:LANES] + product[spot : spot + chunk, LANES:]
                    )
                    along = ahead_share * src(item, w, OFF + at + 1, chunk) + behind_share * src(
                        item, w, OFF + at - 1, chunk
                    )
                    dst(item, w, OFF + at, chunk, mixed + along + 0.1 * (here[one] + here[other]))


def relays_of(lon_count):
    tail_from, half_turn = lon_count // 4 - 1, lon_count // 2
    relays = {dev: [] for dev in (half_turn - 1, lon_count - 1, half_turn)}
    relays[tail_from], relays[half_turn + tail_from] = [], []
    for first, last in ((tail_from, half_turn - 1), (half_turn + tail_from, lon_count - 1)):
        for dev in range(first + 1, last):
            relays[first if dev <= first + 2 else last].append(dev)
    for dev in range(half_turn + 1, half_turn + tail_from):
        relays[dev] = []
    return relays


def kernel(
    counts,
    zlen_ref,
    zs,
    zc,
    owner_ref,
    ms,
    mc,
    mix_ref,
    out_z,
    out_m,
    out_c,
    raw,
    rawc,
    owner,
    mix,
    zlen,
    first,
    state,
    other_state,
    weights,
    strips,
    other_strips,
    scour,
    back,
    edges,
    halos,
    tails,
    gathered,
    gathered_0,
    heads,
    part,
    part_in,
    load_sem,
    send_sem,
    recv_sem,
    far_send,
    far_recv,
):
    lon_count, lat_count = counts
    half_turn = lon_count // 2
    tail_from = lon_count // 4 - 1
    tail_devs = list(range(tail_from, lon_count))
    relays = relays_of(lon_count)
    me, lat = lax.axis_index("lon"), lax.axis_index("lat")
    left = lax.rem(me + lon_count - 1, lon_count)
    right = lax.rem(me + 1, lon_count)
    across = lax.rem(me + half_turn, lon_count)
    at_south, at_north = lat == 0, lat == lat_count - 1
    south = {"lon": jnp.where(at_south, across, me), "lat": jnp.where(at_south, lat, lat - 1)}
    north = {"lon": jnp.where(at_north, across, me), "lat": jnp.where(at_north, lat, lat + 1)}
    west, east = {"lon": left, "lat": lat}, {"lon": right, "lat": lat}
    root = {"lon": 0 * me, "lat": lat}
    is_root, is_tail, is_half = me == 0, me >= tail_from, me == half_turn

    barrier = pltpu.get_barrier_semaphore()
    for peer in (west, east, south, north):
        pl.semaphore_signal(barrier, inc=1, device_id=peer, device_id_type=MESH)

    def sector(dev):
        return {"lon": 0 * me + dev, "lat": lat}

    child_count = 0 * me
    for relay, children in relays.items():
        child_count = child_count + jnp.where(me == relay, len(children), 0)

        @pl.when(me == relay)
        def _():
            pl.semaphore_signal(barrier, inc=1, device_id=root, device_id_type=MESH)

        if children:

            @pl.when((me >= children[0]) & (me <= children[-1]))
            def _(relay=relay):
                pl.semaphore_signal(
                    barrier, inc=1, device_id=sector(relay), device_id_type=MESH
                )

    peers = 4 + jnp.where(is_tail, 1, 0) + child_count + jnp.where(is_root, len(relays), 0)

    @pl.when(is_root)
    def _():
        for dev in tail_devs:
            pl.semaphore_signal(
                barrier, inc=1, device_id={"lon": 0 * me + dev, "lat": lat}, device_id_type=MESH
            )

    loads = []
    for f, (s_ref, c_ref) in enumerate(((zs, zc), (ms, mc))):
        loads.append(pltpu.make_async_copy(s_ref, raw.at[f], load_sem.at[f, 0]))
        loads.append(pltpu.make_async_copy(c_ref, rawc.at[f], load_sem.at[f, 1]))
    loads.append(pltpu.make_async_copy(mix_ref, mix, load_sem.at[2, 0]))
    loads.append(pltpu.make_async_copy(owner_ref, owner, load_sem.at[2, 1]))
    loads.append(pltpu.make_async_copy(zlen_ref, zlen, load_sem.at[3, 0]))
    for load in loads:
        load.start()

    def turn_in(f, channels):
        if channels[0] != 1:
            loads[2 * f].wait()
            loads[2 * f + 1].wait()
        for r in channels:
            for w in range(3):
                turned = raw[f, pl.ds(w * 4 + r, LANES, stride=12), :].T
                first[4 * f + r, w, OFF : OFF + CELLS, :] = turned
                state[4 * f + r, w, OFF : OFF + CELLS, :] = turned
            c_now = rawc[f, pl.ds(r, 32, stride=4), :]
            first[4 * f + r, 3, OFF : OFF + CELLS, :] = jnp.concatenate([c_now] * 4, axis=0).T
        for r in channels:
            for p in range(4):
                edges[f, 0, r, 4 * p : 4 * p + 4, :] = first[4 * f + r, p, OFF : OFF + SUB, :]
                edges[f, 1, r, 4 * p : 4 * p + 4, :] = first[
                    4 * f + r, p, OFF + CELLS - SUB : OFF + CELLS, :
                ]

    with jax.named_scope("turn_z"):
        turn_in(0, (2, 3, 0))
        loads[6].wait()
        ends = [jnp.clip(zlen[r] - me * CELLS, 0, CELLS + SUB) for r in range(4)]
        quarter = lax.broadcasted_iota(jnp.int32, (8, LANES), 0)
        for r in FAR:
            cell = ends[r] - SUB + quarter
            own = (cell >= 0) & (cell < CELLS)
            for p in range(4):
                found = jnp.where(own, first[r, p, pl.ds(OFF + ends[r] - SUB, 8), :], 0.0)
                tails[r, 4 * p : 4 * p + 4, :] = found[0:SUB]
        turn_in(0, (1,))

    def remote(src, dst, s_sem, r_sem, peer):
        return pltpu.make_async_remote_copy(
            src_ref=src,
            dst_ref=dst,
            send_sem=s_sem,
            recv_sem=r_sem,
            device_id=peer,
            device_id_type=MESH,
        )

    slot = jnp.maximum(me - tail_from, 0)
    tail_copy = remote(
        tails.at[2:4], gathered.at[slot], far_send.at[0], far_recv.at[slot], root
    )
    tail_0_copy = remote(
        tails.at[0], gathered_0, far_send.at[1], recv_sem.at[7], root
    )
    head_copies = [
        remote(
            edges.at[0, 0, 2:4], heads.at[2:4], far_send.at[2 + n], recv_sem.at[8], sector(relay)
        )
        for n, relay in enumerate(relays)
    ]
    head_0_copy = remote(
        edges.at[0, 0, 0], heads.at[0], far_send.at[1], recv_sem.at[9], sector(half_turn)
    )
    passed_on = {
        relay: [
            remote(heads.at[2:4], heads.at[2:4], far_send.at[2 + n], recv_sem.at[8], sector(dev))
            for n, dev in enumerate(children)
        ]
        for relay, children in relays.items()
    }

    south_side, north_side = jnp.where(at_south, 0, 1), jnp.where(at_north, 1, 0)
    near = [
        remote(edges.at[0, 0], halos.at[0, 1], send_sem.at[0], recv_sem.at[1], west),
        remote(edges.at[0, 1], halos.at[0, 0], send_sem.at[1], recv_sem.at[0], east),
        remote(
            edges.at[1, 0],
            halos.at[1, south_side],
            send_sem.at[2],
            recv_sem.at[2 + south_side],
            south,
        ),
        remote(
            edges.at[1, 1],
            halos.at[1, north_side],
            send_sem.at[3],
            recv_sem.at[2 + north_side],
            north,
        ),
    ]
    place = lax.rem(me, half_turn)
    is_late, is_early, is_mid = place >= half_turn // 2, place == 0, place == tail_from

    def entered():
        with jax.named_scope("barrier"):
            pl.semaphore_wait(barrier, peers)

        @pl.when(is_tail)
        def _():
            tail_copy.start()

        @pl.when(is_half)
        def _():
            tail_0_copy.start()

        for copy in near[:2]:
            copy.start()

    def then_send():
        for copy in near[2:]:
            copy.start()

        @pl.when(is_root)
        def _():
            for copy in head_copies:
                copy.start()
            head_0_copy.start()

    @pl.when(jnp.logical_not(is_early | is_mid))
    def _():
        entered()

    with jax.named_scope("turn_m"):
        turn_in(1, (0, 1, 2, 3))

    loads[4].wait()
    loads[5].wait()
    spread = jnp.concatenate([mix[...]] * 4, axis=1)
    row_at = lax.broadcasted_iota(jnp.int32, (LANES, LANES), 0)
    lane_at = lax.broadcasted_iota(jnp.int32, (LANES, LANES), 1)
    spread = jnp.where(row_at // 32 == lane_at // 32, spread, 0.0)
    spread = spread + jnp.where(row_at == lane_at, 0.2, 0.0)
    high, low = two_parts(spread.T)
    for row in (0, LANES):
        weights[row : row + LANES, 0:LANES] = high
        weights[row : row + LANES, LANES:] = low

    def one_way(there, back, courant, items, rows, chunk):
        def src(item, w, at, size):
            return there[item, w, pl.ds(at, size), :]

        def dst(item, w, at, size, value):
            back[item, w, pl.ds(at, size), :] = value

        advance(src, dst, courant, weights, items, rows, chunk)

    def two_steps(there, back, courant, items, rows, chunk):
        one_way(there, back, courant, items, rows, chunk)
        one_way(back, there, courant, items, rows, chunk)

    def interior(f):
        items = [4 * f + r for r in range(4)]

        def courant(ch, at, size):
            return first[ch, 3, pl.ds(OFF + at, size), :]

        def step(t, carry):
            two_steps(state, other_state, courant, items, CELLS, 16)
            return carry

        lax.fori_loop(0, SUB // 2, step, 0)

    def arrived(f, side):
        pltpu.make_async_copy(
            halos.at[f, side], halos.at[f, side], recv_sem.at[2 * f + side]
        ).wait()

    def strip_steps(count):
        def step(t, carry):
            two_steps(
                strips,
                other_strips,
                lambda n, at, size: scour[n, pl.ds(at, size), :],
                list(range(count)),
                WIN,
                16,
            )
            return carry

        lax.fori_loop(0, SUB // 2, step, 0)

    def fill(n, ch, start):
        for w in range(3):
            strips[n, w, OFF : OFF + WIN, :] = first[ch, w, pl.ds(start, WIN), :]
        scour[n, :, :] = first[ch, 3, pl.ds(start, WIN), :]

    left_row, right_row = OFF - SUB, OFF + CELLS
    left_start, right_start = OFF - SUB, OFF + CELLS + SUB - WIN
    near_columns = me * GLON_DEV - 1 + lax.broadcasted_iota(jnp.int32, (8, CELLS), 0)
    column = lax.broadcasted_iota(jnp.int32, (CELLS, LANES), 0)
    scale = GLON_DEV / (3.0 * CELLS)
    back_copy = remote(part.at[4], part_in.at[1], send_sem.at[4], recv_sem.at[5], west)
    on_copy = remote(part.at[5], part_in.at[0], send_sem.at[5], recv_sem.at[4], east)
    is_last = me == lon_count - 1

    def merid_end():
        with jax.named_scope("merid_wait"):
            arrived(1, 0)
            arrived(1, 1)
        for side, turned, row in ((0, at_south, left_row), (1, at_north, right_row)):
            for r in range(4):
                for p in range(4):
                    plain = halos[1, side, r, 4 * p : 4 * p + 4, :]
                    q = p if p == 3 else 2 - p
                    mirrored = jnp.concatenate(
                        [halos[1, side, r, 4 * q + 3 - j : 4 * q + 4 - j, :] for j in range(SUB)],
                        axis=0,
                    )
                    if p == 3:
                        mirrored = -mirrored
                    first[4 + r, p, row : row + SUB, :] = jnp.where(turned, mirrored, plain)
        for r in range(4):
            fill(r, 4 + r, left_start)
            fill(4 + r, 4 + r, right_start)
        with jax.named_scope("merid_strips"):
            strip_steps(8)
        for r in range(4):
            for w in range(3):
                kept = strips[r, w, OFF + 4 : OFF + 8, :]
                state[4 + r, w, OFF : OFF + SUB, :] = kept
                kept = strips[4 + r, w, OFF + 8 : OFF + 12, :]
                state[4 + r, w, OFF + CELLS - SUB : OFF + CELLS, :] = kept
        for r in range(4):
            for w in range(3):
                out_m[pl.ds(w * 4 + r, LANES, stride=12), :] = state[
                    4 + r, w, OFF : OFF + CELLS, :
                ].T

    def shares(r, change):
        high, low = two_parts(change * scale)
        mine = (jnp.broadcast_to(owner[r : r + 1, :], (8, CELLS)) == near_columns).astype(BF16)
        return jnp.dot(
            jnp.concatenate([mine, mine], axis=1),
            jnp.concatenate([high, low], axis=0),
            preferred_element_type=F32,
        )

    def right_strips(at):
        for r in range(4):
            for p in range(4):
                first[r, p, right_row : right_row + SUB, :] = halos[0, 1, r, 4 * p : 4 * p + 4, :]
        for r in range(4):
            fill(at + r, r, right_start)

    def right_kept(at):
        for r in range(4):
            for w in range(3):
                kept = strips[at + r, w, OFF + 8 : OFF + 12, :]
                state[r, w, OFF + CELLS - SUB : OFF + CELLS, :] = kept

    is_relay = functools.reduce(jnp.logical_or, [me == relay for relay in relays])

    def heads_arrived():
        pltpu.make_async_copy(heads.at[2:4], heads.at[2:4], recv_sem.at[8]).wait()

    def pass_on():
        with jax.named_scope("pass_on"):
            for relay, copies in passed_on.items():

                @pl.when(me == relay)
                def _(copies=copies):
                    heads_arrived()
                    for copy in copies:
                        copy.start()

    def early_part():
        arrived(0, 1)
        with jax.named_scope("early_part"):
            right_strips(0)
            strip_steps(4)
            right_kept(0)
            for r in range(4):
                change = None
                for w in range(3):
                    value = (
                        state[r, w, OFF : OFF + CELLS, :] - first[r, w, OFF : OFF + CELLS, :]
                    )
                    change = value if change is None else change + value
                change = jnp.where(column >= SUB, change, 0.0)
                part[5, r : r + 1, :] = shares(r, change)[5:6]
            on_copy.start()

    def zonal_end(first_wait=True):
        if first_wait:
            with jax.named_scope("right_wait"):
                arrived(0, 1)

        with jax.named_scope("far_wait"):

            arrived(0, 0)

            @pl.when(is_tail & jnp.logical_not(is_relay))
            def _():
                heads_arrived()

            @pl.when(is_half)
            def _():
                pltpu.make_async_copy(heads.at[0], heads.at[0], recv_sem.at[9]).wait()

            @pl.when(is_root)
            def _():
                for n in range(len(tail_devs)):
                    pltpu.make_async_copy(gathered.at[n], gathered.at[n], far_recv.at[n]).wait()
                pltpu.make_async_copy(gathered_0, gathered_0, recv_sem.at[7]).wait()

        for r in range(4):
            for p in range(4):
                first[r, p, left_row : left_row + SUB, :] = halos[0, 0, r, 4 * p : 4 * p + 4, :]

        @pl.when(is_root)
        def _():
            for r in FAR:
                if r == 0:
                    tail_cells = gathered_0[...]
                else:
                    tail_cells = gathered[0, r - 2]
                    for n in range(1, len(tail_devs)):
                        tail_cells = tail_cells + gathered[n, r - 2]
                for p in range(4):
                    first[r, p, left_row : left_row + SUB, :] = tail_cells[4 * p : 4 * p + 4]

        right_strips(0)
        for r in range(4):
            fill(4 + r, r, left_start)
        for n, r in enumerate(FAR):
            fill(8 + n, r, ends[r])
            for w in range(3):
                strips[8 + n, w, OFF + 8 : OFF + 12, :] = heads[r, 4 * w : 4 * w + 4, :]
            scour[8 + n, 8:12, :] = heads[r, 12:16, :]
        with jax.named_scope("zonal_strips"):
            strip_steps(11)
        right_kept(0)
        for r in range(4):
            for w in range(3):
                kept = strips[4 + r, w, OFF + 4 : OFF + 8, :]
                state[r, w, OFF : OFF + SUB, :] = kept
        for n, r in enumerate(FAR):
            for w in range(3):
                back[n, w, PBASE : PBASE + WIN, :] = strips[8 + n, w, OFF : OFF + WIN, :]

        for r in range(4):
            change = None
            for w in range(3):
                value = state[r, w, OFF : OFF + CELLS, :]
                before = first[r, w, OFF : OFF + CELLS, :]
                if r in FAR:
                    n = FAR.index(r)
                    cut = ends[r]
                    strip = back[n, w, pl.ds(PBASE + 8 - cut, CELLS), :]
                    value = jnp.where(column >= cut - SUB, strip, value)
                    value = jnp.where(column < cut, value, before)
                    state[r, w, OFF : OFF + CELLS, :] = value
                change = value - before if change is None else change + (value - before)
            part[r, :, :] = shares(r, change)

        @pl.when(jnp.logical_not(is_root))
        def _():
            for r in range(4):
                part[4, r : r + 1, :] = part[r, 0:1, :]
            back_copy.start()

        @pl.when(jnp.logical_not(is_root | is_last))
        def _():
            for r in range(4):
                part[5, r : r + 1, :] = part[r, 5:6, :]
            on_copy.start()

    @pl.when(jnp.logical_not(is_early | is_mid))
    def _():
        then_send()

    @pl.when(is_late)
    def _():
        with jax.named_scope("interior_z"):
            interior(0)
        pass_on()
        zonal_end()
        with jax.named_scope("interior_m"):
            interior(1)
        merid_end()

    @pl.when(jnp.logical_not(is_late))
    def _():
        with jax.named_scope("interior_m"):
            interior(1)

        @pl.when(is_mid)
        def _():
            entered()
            then_send()

        with jax.named_scope("interior_z"):
            interior(0)

        @pl.when(is_early)
        def _():
            entered()
            then_send()

        @pl.when(is_root)
        def _():
            early_part()

        @pl.when(jnp.logical_not(is_root))
        def _():
            with jax.named_scope("right_wait"):
                arrived(0, 1)

        @pl.when(jnp.logical_not(is_early | is_mid) | is_root)
        def _():
            merid_end()

        pass_on()
        zonal_end(False)

        @pl.when((is_early | is_mid) & jnp.logical_not(is_root))
        def _():
            merid_end()

    for r in range(4):
        for w in range(3):
            out_z[pl.ds(w * 4 + r, LANES, stride=12), :] = state[r, w, OFF : OFF + CELLS, :].T

    with jax.named_scope("part_wait"):

        @pl.when(is_root)
        def _():
            part_in[0, :, :] = jnp.zeros((8, LANES), F32)

        @pl.when(is_last)
        def _():
            part_in[1, :, :] = jnp.zeros((8, LANES), F32)

        @pl.when(jnp.logical_not(is_last))
        def _():
            back_copy.wait_recv()

        @pl.when(jnp.logical_not(is_root))
        def _():
            on_copy.wait_recv()

    for r in range(4):
        for g in range(GLON_DEV):
            value = part[r, g + 1 : g + 2, :]
            if g == 0:
                value = value + part_in[0, r : r + 1, :]
            if g == GLON_DEV - 1:
                value = value + part_in[1, r : r + 1, :]
            out_c[4 * g + r : 4 * g + r + 1, :] = value

    for copy in near:
        copy.wait_send()

    @pl.when(jnp.logical_not(is_root))
    def _():
        back_copy.wait_send()

    @pl.when(jnp.logical_not(is_last))
    def _():
        on_copy.wait_send()

    @pl.when(is_tail)
    def _():
        tail_copy.wait_send()

    @pl.when(is_half)
    def _():
        tail_0_copy.wait_send()

    for relay, copies in passed_on.items():

        @pl.when(me == relay)
        def _(copies=copies):
            for copy in copies:
                copy.wait_send()

    @pl.when(is_root)
    def _():
        head_0_copy.wait_send()
        for copy in head_copies:
            copy.wait_send()


def write_out(z, m, c, out_z, out_m, out_c, sem):
    copies = [
        pltpu.make_async_copy(src, dst, sem.at[n])
        for n, (src, dst) in enumerate(((z, out_z), (m, out_m), (c, out_c)))
    ]
    for copy in copies:
        copy.start()
    for copy in copies:
        copy.wait()


def shards(
    counts, zonal_state, zonal_courant, zonal_length, zonal_owner, merid_state, merid_courant, mixing
):
    tail_count = counts[0] - (counts[0] // 4 - 1)
    relays = relays_of(counts[0])
    hbm = pl.BlockSpec(memory_space=pltpu.HBM)
    vmem = pl.BlockSpec(memory_space=pltpu.VMEM)
    flat_shape = (LANES * 12, CELLS)

    def in_hbm(array, shape):
        return pltpu.with_memory_space_constraint(array.reshape(shape), pltpu.HBM)

    out_z, out_m, out_c = pl.pallas_call(
        functools.partial(kernel, counts),
        out_shape=(
            pltpu.VMEM(flat_shape, F32),
            pltpu.VMEM(flat_shape, F32),
            pltpu.VMEM((4 * GLON_DEV, LANES), F32),
        ),
        in_specs=[hbm, hbm, hbm, hbm, hbm, hbm, hbm],
        out_specs=(vmem, vmem, vmem),
        scratch_shapes=[
            pltpu.VMEM((2, *flat_shape), F32),
            pltpu.VMEM((2, LANES, CELLS), F32),
            pltpu.VMEM((4, CELLS), jnp.int32),
            pltpu.VMEM((LANES, 32), F32),
            pltpu.SMEM((4,), jnp.int32),
            pltpu.VMEM((8, 4, ROWS, LANES), F32),
            pltpu.VMEM((8, 3, ROWS, LANES), F32),
            pltpu.VMEM((8, 3, ROWS, LANES), F32),
            pltpu.VMEM((2 * LANES, 2 * LANES), BF16),
            pltpu.VMEM((12, 3, SROWS, LANES), F32),
            pltpu.VMEM((12, 3, SROWS, LANES), F32),
            pltpu.VMEM((12, WIN, LANES), F32),
            pltpu.VMEM((3, 3, PROWS, LANES), F32),
            pltpu.VMEM((2, 2, 4, 16, LANES), F32),
            pltpu.VMEM((2, 2, 4, 16, LANES), F32),
            pltpu.VMEM((4, 16, LANES), F32),
            pltpu.VMEM((tail_count, 2, 16, LANES), F32),
            pltpu.VMEM((16, LANES), F32),
            pltpu.VMEM((4, 16, LANES), F32),
            pltpu.VMEM((6, 8, LANES), F32),
            pltpu.VMEM((2, 8, LANES), F32),
            pltpu.SemaphoreType.DMA((4, 2)),
            pltpu.SemaphoreType.DMA((6,)),
            pltpu.SemaphoreType.DMA((10,)),
            pltpu.SemaphoreType.DMA((2 + max(map(len, (relays, *relays.values()))),)),
            pltpu.SemaphoreType.DMA((tail_count,)),
        ],
        compiler_params=pltpu.CompilerParams(
            collective_id=0, has_side_effects=True, vmem_limit_bytes=32 * 1024 * 1024
        ),
    )(
        in_hbm(zonal_length, (4,)),
        in_hbm(zonal_state, flat_shape),
        in_hbm(zonal_courant, (LANES, CELLS)),
        in_hbm(zonal_owner, (4, CELLS)),
        in_hbm(merid_state, flat_shape),
        in_hbm(merid_courant, (LANES, CELLS)),
        in_hbm(mixing, (LANES, 32)),
    )
    out_z, out_m, out_c = pl.pallas_call(
        write_out,
        out_shape=(
            pltpu.HBM(flat_shape, F32),
            pltpu.HBM(flat_shape, F32),
            pltpu.HBM((4 * GLON_DEV, LANES), F32),
        ),
        in_specs=[vmem, vmem, vmem],
        out_specs=(hbm, hbm, hbm),
        scratch_shapes=[pltpu.SemaphoreType.DMA((3,))],
        compiler_params=pltpu.CompilerParams(vmem_limit_bytes=1024 * 1024),
    )(out_z, out_m, out_c)
    return (
        out_z.reshape(zonal_state.shape),
        out_m.reshape(merid_state.shape),
        out_c.reshape(GLON_DEV, 4, LANES),
    )


def solution(mesh):
    counts = (mesh.shape["lon"], mesh.shape["lat"])
    return jax.shard_map(
        functools.partial(shards, counts),
        mesh=mesh,
        in_specs=(
            P(None, None, None, "lat", "lon"),
            P(None, "lat", "lon"),
            P("lat"),
            P("lat", "lon"),
            P(None, None, None, "lon", "lat"),
            P(None, "lon", "lat"),
            P(),
        ),
        out_specs=(
            P(None, None, None, "lat", "lon"),
            P(None, None, None, "lon", "lat"),
            P("lon", "lat", None),
        ),
        check_vma=False,
    )
```

```python
import functools

import jax
import jax.numpy as jnp
from jax import lax
from jax.experimental import pallas as pl
from jax.experimental.pallas import tpu as pltpu
from jax.sharding import PartitionSpec as P

SUB = 4
OFF = 8
CELLS = 128
LANES = 128
ROWS = 152
WIN = 16
SROWS = 32
PROWS = 272
PBASE = 136
GLON_DEV = 4
FAR = (0, 2, 3)
MESH = pl.DeviceIdType.MESH
F32 = jnp.float32
BF16 = jnp.bfloat16


def two_parts(value):
    high = value.astype(BF16)
    low = (value - high.astype(F32)).astype(BF16)
    return high, low


def advance(src, dst, courant, weights, items, rows, chunk):
    group = max(1, CELLS // rows)
    for first_item in range(0, len(items), group):
        some = items[first_item : first_item + group]
        parts = [
            jnp.concatenate(two_parts(src(item, w, OFF, rows)), axis=1)
            for item in some
            for w in range(3)
        ]
        product = jnp.dot(
            jnp.concatenate(parts, axis=0), weights[...], preferred_element_type=F32
        )
        for n, item in enumerate(some):
            for at in range(0, rows, chunk):
                half = 0.5 * courant(item, at, chunk)
                ahead_share, behind_share = 0.3 - half, 0.3 + half
                here = [src(item, w, OFF + at, chunk) for w in range(3)]
                for w, (one, other) in enumerate(((0, 1), (0, 2), (1, 2))):
                    spot = (n * 3 + w) * rows + at
                    mixed = (
                        product[spot : spot + chunk, 0:LANES] + product[spot : spot + chunk, LANES:]
                    )
                    along = ahead_share * src(item, w, OFF + at + 1, chunk) + behind_share * src(
                        item, w, OFF + at - 1, chunk
                    )
                    dst(item, w, OFF + at, chunk, mixed + along + 0.1 * (here[one] + here[other]))


def relays_of(lon_count):
    tail_from, half_turn = lon_count // 4 - 1, lon_count // 2
    relays = {dev: [] for dev in (half_turn - 1, lon_count - 1, half_turn)}
    relays[tail_from], relays[half_turn + tail_from] = [], []
    for first, last in ((tail_from, half_turn - 1), (half_turn + tail_from, lon_count - 1)):
        for dev in range(first + 1, last):
            relays[first if dev <= first + 2 else last].append(dev)
    for dev in range(half_turn + 1, half_turn + tail_from):
        relays[dev] = []
    return relays


def kernel(
    counts,
    zlen_ref,
    zs,
    zc,
    owner_ref,
    ms,
    mc,
    mix_ref,
    out_z,
    out_m,
    out_c,
    raw,
    rawc,
    owner,
    mix,
    zlen,
    first,
    state,
    other_state,
    weights,
    strips,
    other_strips,
    scour,
    back,
    edges,
    halos,
    tails,
    gathered,
    gathered_0,
    heads,
    part,
    part_in,
    load_sem,
    send_sem,
    recv_sem,
    far_send,
    far_recv,
    entry_sem,
):
    lon_count, lat_count = counts
    half_turn = lon_count // 2
    tail_from = lon_count // 4 - 1
    tail_devs = list(range(tail_from, lon_count))
    relays = relays_of(lon_count)
    me, lat = lax.axis_index("lon"), lax.axis_index("lat")
    left = lax.rem(me + lon_count - 1, lon_count)
    right = lax.rem(me + 1, lon_count)
    across = lax.rem(me + half_turn, lon_count)
    at_south, at_north = lat == 0, lat == lat_count - 1
    south = {"lon": jnp.where(at_south, across, me), "lat": jnp.where(at_south, lat, lat - 1)}
    north = {"lon": jnp.where(at_north, across, me), "lat": jnp.where(at_north, lat, lat + 1)}
    west, east = {"lon": left, "lat": lat}, {"lon": right, "lat": lat}
    root = {"lon": 0 * me, "lat": lat}
    is_root, is_tail, is_half = me == 0, me >= tail_from, me == half_turn

    loads = []
    for f, (s_ref, c_ref) in enumerate(((zs, zc), (ms, mc))):
        loads.append(pltpu.make_async_copy(s_ref, raw.at[f], load_sem.at[f, 0]))
        loads.append(pltpu.make_async_copy(c_ref, rawc.at[f], load_sem.at[f, 1]))
    loads.append(pltpu.make_async_copy(mix_ref, mix, load_sem.at[2, 0]))
    loads.append(pltpu.make_async_copy(owner_ref, owner, load_sem.at[2, 1]))
    loads.append(pltpu.make_async_copy(zlen_ref, zlen, load_sem.at[3, 0]))
    for load in loads:
        load.start()

    place = lax.rem(me, half_turn)
    is_late, is_early, is_mid = place >= half_turn // 2, place == 0, place == tail_from
    answers = is_late & (lat == lat_count // 2 - 1)
    asks = is_late & (lat == lat_count // 2)

    barrier = pltpu.get_barrier_semaphore()
    for peer in (west, east, south):
        pl.semaphore_signal(barrier, inc=1, device_id=peer, device_id_type=MESH)

    @pl.when(jnp.logical_not(answers))
    def _():
        pl.semaphore_signal(barrier, inc=1, device_id=north, device_id_type=MESH)

    def sector(dev):
        return {"lon": 0 * me + dev, "lat": lat}

    child_count = 0 * me
    for relay, children in relays.items():
        child_count = child_count + jnp.where(me == relay, len(children), 0)

        @pl.when(me == relay)
        def _():
            pl.semaphore_signal(barrier, inc=1, device_id=root, device_id_type=MESH)

        if children:

            @pl.when((me >= children[0]) & (me <= children[-1]))
            def _(relay=relay):
                pl.semaphore_signal(
                    barrier, inc=1, device_id=sector(relay), device_id_type=MESH
                )

    zonal_first = (is_early | is_mid | (me < tail_from)) & (me != 0)
    peers = 4 - jnp.where(asks, 1, 0) + jnp.where(is_tail, 1, 0) + child_count + jnp.where(is_root, len(relays), 0)

    @pl.when(is_root)
    def _():
        for dev in tail_devs:
            pl.semaphore_signal(
                barrier, inc=1, device_id={"lon": 0 * me + dev, "lat": lat}, device_id_type=MESH
            )

    def turn_in(f, channels):
        if channels[0] != 1:
            loads[2 * f].wait()
            loads[2 * f + 1].wait()
        for r in channels:
            for w in range(3):
                turned = raw[f, pl.ds(w * 4 + r, LANES, stride=12), :].T
                first[4 * f + r, w, OFF : OFF + CELLS, :] = turned
                state[4 * f + r, w, OFF : OFF + CELLS, :] = turned
            c_now = rawc[f, pl.ds(r, 32, stride=4), :]
            first[4 * f + r, 3, OFF : OFF + CELLS, :] = jnp.concatenate([c_now] * 4, axis=0).T
        for r in channels:
            for p in range(4):
                edges[f, 0, r, 4 * p : 4 * p + 4, :] = first[4 * f + r, p, OFF : OFF + SUB, :]
                edges[f, 1, r, 4 * p : 4 * p + 4, :] = first[
                    4 * f + r, p, OFF + CELLS - SUB : OFF + CELLS, :
                ]

    with jax.named_scope("turn_z"):
        turn_in(0, (2, 3, 0))
        loads[6].wait()
        ends = [jnp.clip(zlen[r] - me * CELLS, 0, CELLS + SUB) for r in range(4)]
        quarter = lax.broadcasted_iota(jnp.int32, (8, LANES), 0)
        for r in FAR:
            cell = ends[r] - SUB + quarter
            own = (cell >= 0) & (cell < CELLS)
            for p in range(4):
                found = jnp.where(own, first[r, p, pl.ds(OFF + ends[r] - SUB, 8), :], 0.0)
                tails[r, 4 * p : 4 * p + 4, :] = found[0:SUB]
        turn_in(0, (1,))

    def remote(src, dst, s_sem, r_sem, peer):
        return pltpu.make_async_remote_copy(
            src_ref=src,
            dst_ref=dst,
            send_sem=s_sem,
            recv_sem=r_sem,
            device_id=peer,
            device_id_type=MESH,
        )

    slot = jnp.maximum(me - tail_from, 0)
    tail_copy = remote(
        tails.at[2:4], gathered.at[slot], far_send.at[0], far_recv.at[slot], root
    )
    tail_0_copy = remote(
        tails.at[0], gathered_0, far_send.at[1], recv_sem.at[7], root
    )
    head_copies = [
        remote(
            edges.at[0, 0, 2:4], heads.at[2:4], far_send.at[2 + n], recv_sem.at[8], sector(relay)
        )
        for n, relay in enumerate(relays)
    ]
    head_0_copy = remote(
        edges.at[0, 0, 0], heads.at[0], far_send.at[1], recv_sem.at[9], sector(half_turn)
    )
    passed_on = {
        relay: [
            remote(heads.at[2:4], heads.at[2:4], far_send.at[2 + n], recv_sem.at[8], sector(dev))
            for n, dev in enumerate(children)
        ]
        for relay, children in relays.items()
    }

    south_side, north_side = jnp.where(at_south, 0, 1), jnp.where(at_north, 1, 0)
    near = [
        remote(edges.at[0, 0], halos.at[0, 1], send_sem.at[0], recv_sem.at[1], west),
        remote(edges.at[0, 1], halos.at[0, 0], send_sem.at[1], recv_sem.at[0], east),
        remote(
            edges.at[1, 0],
            halos.at[1, south_side],
            send_sem.at[2],
            recv_sem.at[2 + south_side],
            south,
        ),
        remote(
            edges.at[1, 1],
            halos.at[1, north_side],
            send_sem.at[3],
            recv_sem.at[2 + north_side],
            north,
        ),
    ]
    def entered(first_send=None):
        with jax.named_scope("barrier"):
            pl.semaphore_wait(barrier, peers)

        if first_send is not None:
            first_send()

        @pl.when(answers)
        def _():
            pl.semaphore_signal(entry_sem, inc=1, device_id=north, device_id_type=MESH)

        @pl.when(is_tail)
        def _():
            tail_copy.start()

        @pl.when(is_half)
        def _():
            tail_0_copy.start()

        for copy in near[:2]:
            copy.start()

        @pl.when(is_root)
        def _():
            for copy in head_copies:
                copy.start()
            head_0_copy.start()

    def then_send():
        near[3].start()

        @pl.when(jnp.logical_not(asks))
        def _():
            near[2].start()

    @pl.when(jnp.logical_not(is_early | is_mid))
    def _():
        entered()

    with jax.named_scope("turn_m"):
        turn_in(1, (0, 1, 2, 3))

    loads[4].wait()
    loads[5].wait()
    spread = jnp.concatenate([mix[...]] * 4, axis=1)
    row_at = lax.broadcasted_iota(jnp.int32, (LANES, LANES), 0)
    lane_at = lax.broadcasted_iota(jnp.int32, (LANES, LANES), 1)
    spread = jnp.where(row_at // 32 == lane_at // 32, spread, 0.0)
    spread = spread + jnp.where(row_at == lane_at, 0.2, 0.0)
    high, low = two_parts(spread.T)
    for row in (0, LANES):
        weights[row : row + LANES, 0:LANES] = high
        weights[row : row + LANES, LANES:] = low

    def one_way(there, back, courant, items, rows, chunk):
        def src(item, w, at, size):
            return there[item, w, pl.ds(at, size), :]

        def dst(item, w, at, size, value):
            back[item, w, pl.ds(at, size), :] = value

        advance(src, dst, courant, weights, items, rows, chunk)

    def two_steps(there, back, courant, items, rows, chunk):
        one_way(there, back, courant, items, rows, chunk)
        one_way(back, there, courant, items, rows, chunk)

    def interior(f):
        items = [4 * f + r for r in range(4)]

        def courant(ch, at, size):
            return first[ch, 3, pl.ds(OFF + at, size), :]

        def step(t, carry):
            two_steps(state, other_state, courant, items, CELLS, 16)
            return carry

        lax.fori_loop(0, SUB // 2, step, 0)

    def arrived(f, side):
        pltpu.make_async_copy(
            halos.at[f, side], halos.at[f, side], recv_sem.at[2 * f + side]
        ).wait()

    def strip_steps(count):
        def step(t, carry):
            two_steps(
                strips,
                other_strips,
                lambda n, at, size: scour[n, pl.ds(at, size), :],
                list(range(count)),
                WIN,
                16,
            )
            return carry

        lax.fori_loop(0, SUB // 2, step, 0)

    def fill(n, ch, start):
        for w in range(3):
            strips[n, w, OFF : OFF + WIN, :] = first[ch, w, pl.ds(start, WIN), :]
        scour[n, :, :] = first[ch, 3, pl.ds(start, WIN), :]

    left_row, right_row = OFF - SUB, OFF + CELLS
    left_start, right_start = OFF - SUB, OFF + CELLS + SUB - WIN
    near_columns = me * GLON_DEV - 1 + lax.broadcasted_iota(jnp.int32, (8, CELLS), 0)
    column = lax.broadcasted_iota(jnp.int32, (CELLS, LANES), 0)
    scale = GLON_DEV / (3.0 * CELLS)
    back_copy = remote(part.at[4], part_in.at[1], send_sem.at[4], recv_sem.at[5], west)
    on_copy = remote(part.at[5], part_in.at[0], send_sem.at[5], recv_sem.at[4], east)
    is_last = me == lon_count - 1

    def merid_end():
        with jax.named_scope("merid_wait"):
            arrived(1, 0)
            arrived(1, 1)
        for side, turned, row in ((0, at_south, left_row), (1, at_north, right_row)):
            for r in range(4):
                for p in range(4):
                    plain = halos[1, side, r, 4 * p : 4 * p + 4, :]
                    q = p if p == 3 else 2 - p
                    mirrored = jnp.concatenate(
                        [halos[1, side, r, 4 * q + 3 - j : 4 * q + 4 - j, :] for j in range(SUB)],
                        axis=0,
                    )
                    if p == 3:
                        mirrored = -mirrored
                    first[4 + r, p, row : row + SUB, :] = jnp.where(turned, mirrored, plain)
        for r in range(4):
            fill(r, 4 + r, left_start)
            fill(4 + r, 4 + r, right_start)
        with jax.named_scope("merid_strips"):
            strip_steps(8)
        for r in range(4):
            for w in range(3):
                kept = strips[r, w, OFF + 4 : OFF + 8, :]
                state[4 + r, w, OFF : OFF + SUB, :] = kept
                kept = strips[4 + r, w, OFF + 8 : OFF + 12, :]
                state[4 + r, w, OFF + CELLS - SUB : OFF + CELLS, :] = kept
        for r in range(4):
            for w in range(3):
                out_m[pl.ds(w * 4 + r, LANES, stride=12), :] = state[
                    4 + r, w, OFF : OFF + CELLS, :
                ].T

    def shares(r, change):
        high, low = two_parts(change * scale)
        mine = (jnp.broadcast_to(owner[r : r + 1, :], (8, CELLS)) == near_columns).astype(BF16)
        return jnp.dot(
            jnp.concatenate([mine, mine], axis=1),
            jnp.concatenate([high, low], axis=0),
            preferred_element_type=F32,
        )

    def right_strips(at):
        for r in range(4):
            for p in range(4):
                first[r, p, right_row : right_row + SUB, :] = halos[0, 1, r, 4 * p : 4 * p + 4, :]
        for r in range(4):
            fill(at + r, r, right_start)

    def right_kept(at):
        for r in range(4):
            for w in range(3):
                kept = strips[at + r, w, OFF + 8 : OFF + 12, :]
                state[r, w, OFF + CELLS - SUB : OFF + CELLS, :] = kept

    is_relay = functools.reduce(jnp.logical_or, [me == relay for relay in relays])

    def heads_arrived():
        pltpu.make_async_copy(heads.at[2:4], heads.at[2:4], recv_sem.at[8]).wait()

    def pass_on():
        with jax.named_scope("pass_on"):
            for relay, copies in passed_on.items():

                @pl.when(me == relay)
                def _(copies=copies):
                    heads_arrived()
                    for copy in copies:
                        copy.start()

    def left_kept(at):
        for r in range(4):
            for w in range(3):
                kept = strips[at + r, w, OFF + 4 : OFF + 8, :]
                state[r, w, OFF : OFF + SUB, :] = kept

    def early_part():
        arrived(0, 1)
        with jax.named_scope("early_part"):
            right_strips(0)
            strip_steps(4)
            right_kept(0)
            for r in range(4):
                change = None
                for w in range(3):
                    value = (
                        state[r, w, OFF : OFF + CELLS, :] - first[r, w, OFF : OFF + CELLS, :]
                    )
                    change = value if change is None else change + value
                change = jnp.where(column >= SUB, change, 0.0)
                part[5, r : r + 1, :] = shares(r, change)[5:6]
            on_copy.start()

    def zonal_end(first_wait=True):
        if first_wait:
            with jax.named_scope("right_wait"):
                arrived(0, 1)

        with jax.named_scope("left_wait"):
            arrived(0, 0)
        for r in range(4):
            for p in range(4):
                first[r, p, left_row : left_row + SUB, :] = halos[0, 0, r, 4 * p : 4 * p + 4, :]
        right_strips(0)
        for r in range(4):
            fill(4 + r, r, left_start)
        with jax.named_scope("zonal_strips"):
            strip_steps(8)
        right_kept(0)
        left_kept(4)

        @pl.when(is_tail)
        def _():
            with jax.named_scope("far_wait"):

                @pl.when(jnp.logical_not(is_relay))
                def _():
                    heads_arrived()

                @pl.when(is_half)
                def _():
                    pltpu.make_async_copy(heads.at[0], heads.at[0], recv_sem.at[9]).wait()

            for n, r in enumerate(FAR):
                fill(n, r, ends[r])
                for w in range(3):
                    strips[n, w, OFF + 8 : OFF + 12, :] = heads[r, 4 * w : 4 * w + 4, :]
                scour[n, 8:12, :] = heads[r, 12:16, :]
            with jax.named_scope("far_strips"):
                strip_steps(3)

        @pl.when(is_root)
        def _():
            with jax.named_scope("far_wait"):
                for n in range(len(tail_devs)):
                    pltpu.make_async_copy(gathered.at[n], gathered.at[n], far_recv.at[n]).wait()
                pltpu.make_async_copy(gathered_0, gathered_0, recv_sem.at[7]).wait()
            for r in FAR:
                if r == 0:
                    tail_cells = gathered_0[...]
                else:
                    tail_cells = gathered[0, r - 2]
                    for n in range(1, len(tail_devs)):
                        tail_cells = tail_cells + gathered[n, r - 2]
                for p in range(4):
                    first[r, p, left_row : left_row + SUB, :] = tail_cells[4 * p : 4 * p + 4]
            for r in range(4):
                fill(r, r, left_start)
            with jax.named_scope("far_strips"):
                strip_steps(4)
            left_kept(0)

        for n, r in enumerate(FAR):
            for w in range(3):
                back[n, w, PBASE : PBASE + WIN, :] = strips[n, w, OFF : OFF + WIN, :]

        for r in range(4):
            change = None
            for w in range(3):
                value = state[r, w, OFF : OFF + CELLS, :]
                before = first[r, w, OFF : OFF + CELLS, :]
                if r in FAR:
                    n = FAR.index(r)
                    cut = ends[r]
                    strip = back[n, w, pl.ds(PBASE + 8 - cut, CELLS), :]
                    value = jnp.where(column >= cut - SUB, strip, value)
                    value = jnp.where(column < cut, value, before)
                    state[r, w, OFF : OFF + CELLS, :] = value
                change = value - before if change is None else change + (value - before)
            part[r, :, :] = shares(r, change)

        @pl.when(jnp.logical_not(is_root))
        def _():
            for r in range(4):
                part[4, r : r + 1, :] = part[r, 0:1, :]
            back_copy.start()

        @pl.when(jnp.logical_not(is_root | is_last))
        def _():
            for r in range(4):
                part[5, r : r + 1, :] = part[r, 5:6, :]
            on_copy.start()

    @pl.when(jnp.logical_not(is_early | is_mid))
    def _():
        then_send()

    @pl.when(is_late)
    def _():
        with jax.named_scope("interior_z"):
            interior(0)
        pass_on()

        @pl.when(asks)
        def _():
            with jax.named_scope("answer_wait"):
                pl.semaphore_wait(entry_sem, 1)
            near[2].start()

        zonal_end()
        with jax.named_scope("interior_m"):
            interior(1)
        merid_end()

    @pl.when(jnp.logical_not(is_late))
    def _():
        with jax.named_scope("interior_m"):
            interior(1)

        @pl.when(is_mid | is_early)
        def _():
            entered(then_send)

        with jax.named_scope("interior_z"):
            interior(0)

        @pl.when(is_root)
        def _():
            early_part()

        @pl.when(is_early | is_mid)
        def _():
            pass_on()

        @pl.when(jnp.logical_not(is_root))
        def _():
            with jax.named_scope("right_wait"):
                arrived(0, 1)

        @pl.when(jnp.logical_not(zonal_first))
        def _():
            merid_end()

        @pl.when(jnp.logical_not(is_early | is_mid))
        def _():
            pass_on()

        zonal_end(False)

        @pl.when(zonal_first)
        def _():
            merid_end()

    for r in range(4):
        for w in range(3):
            out_z[pl.ds(w * 4 + r, LANES, stride=12), :] = state[r, w, OFF : OFF + CELLS, :].T

    with jax.named_scope("part_wait"):

        @pl.when(is_root)
        def _():
            part_in[0, :, :] = jnp.zeros((8, LANES), F32)

        @pl.when(is_last)
        def _():
            part_in[1, :, :] = jnp.zeros((8, LANES), F32)

        @pl.when(jnp.logical_not(is_last))
        def _():
            back_copy.wait_recv()

        @pl.when(jnp.logical_not(is_root))
        def _():
            on_copy.wait_recv()

    for r in range(4):
        for g in range(GLON_DEV):
            value = part[r, g + 1 : g + 2, :]
            if g == 0:
                value = value + part_in[0, r : r + 1, :]
            if g == GLON_DEV - 1:
                value = value + part_in[1, r : r + 1, :]
            out_c[4 * g + r : 4 * g + r + 1, :] = value

    for copy in near:
        copy.wait_send()

    @pl.when(jnp.logical_not(is_root))
    def _():
        back_copy.wait_send()

    @pl.when(jnp.logical_not(is_last))
    def _():
        on_copy.wait_send()

    @pl.when(is_tail)
    def _():
        tail_copy.wait_send()

    @pl.when(is_half)
    def _():
        tail_0_copy.wait_send()

    for relay, copies in passed_on.items():

        @pl.when(me == relay)
        def _(copies=copies):
            for copy in copies:
                copy.wait_send()

    @pl.when(is_root)
    def _():
        head_0_copy.wait_send()
        for copy in head_copies:
            copy.wait_send()


def write_out(z, m, c, out_z, out_m, out_c, sem):
    copies = [
        pltpu.make_async_copy(src, dst, sem.at[n])
        for n, (src, dst) in enumerate(((z, out_z), (m, out_m), (c, out_c)))
    ]
    for copy in copies:
        copy.start()
    for copy in copies:
        copy.wait()


def shards(
    counts, zonal_state, zonal_courant, zonal_length, zonal_owner, merid_state, merid_courant, mixing
):
    tail_count = counts[0] - (counts[0] // 4 - 1)
    relays = relays_of(counts[0])
    hbm = pl.BlockSpec(memory_space=pltpu.HBM)
    vmem = pl.BlockSpec(memory_space=pltpu.VMEM)
    flat_shape = (LANES * 12, CELLS)

    def in_hbm(array, shape):
        return pltpu.with_memory_space_constraint(array.reshape(shape), pltpu.HBM)

    out_z, out_m, out_c = pl.pallas_call(
        functools.partial(kernel, counts),
        out_shape=(
            pltpu.VMEM(flat_shape, F32),
            pltpu.VMEM(flat_shape, F32),
            pltpu.VMEM((4 * GLON_DEV, LANES), F32),
        ),
        in_specs=[hbm, hbm, hbm, hbm, hbm, hbm, hbm],
        out_specs=(vmem, vmem, vmem),
        scratch_shapes=[
            pltpu.VMEM((2, *flat_shape), F32),
            pltpu.VMEM((2, LANES, CELLS), F32),
            pltpu.VMEM((4, CELLS), jnp.int32),
            pltpu.VMEM((LANES, 32), F32),
            pltpu.SMEM((4,), jnp.int32),
            pltpu.VMEM((8, 4, ROWS, LANES), F32),
            pltpu.VMEM((8, 3, ROWS, LANES), F32),
            pltpu.VMEM((8, 3, ROWS, LANES), F32),
            pltpu.VMEM((2 * LANES, 2 * LANES), BF16),
            pltpu.VMEM((12, 3, SROWS, LANES), F32),
            pltpu.VMEM((12, 3, SROWS, LANES), F32),
            pltpu.VMEM((12, WIN, LANES), F32),
            pltpu.VMEM((3, 3, PROWS, LANES), F32),
            pltpu.VMEM((2, 2, 4, 16, LANES), F32),
            pltpu.VMEM((2, 2, 4, 16, LANES), F32),
            pltpu.VMEM((4, 16, LANES), F32),
            pltpu.VMEM((tail_count, 2, 16, LANES), F32),
            pltpu.VMEM((16, LANES), F32),
            pltpu.VMEM((4, 16, LANES), F32),
            pltpu.VMEM((6, 8, LANES), F32),
            pltpu.VMEM((2, 8, LANES), F32),
            pltpu.SemaphoreType.DMA((4, 2)),
            pltpu.SemaphoreType.DMA((6,)),
            pltpu.SemaphoreType.DMA((10,)),
            pltpu.SemaphoreType.DMA((2 + max(map(len, (relays, *relays.values()))),)),
            pltpu.SemaphoreType.DMA((tail_count,)),
            pltpu.SemaphoreType.REGULAR,
        ],
        compiler_params=pltpu.CompilerParams(
            collective_id=0, has_side_effects=True, vmem_limit_bytes=32 * 1024 * 1024
        ),
    )(
        in_hbm(zonal_length, (4,)),
        in_hbm(zonal_state, flat_shape),
        in_hbm(zonal_courant, (LANES, CELLS)),
        in_hbm(zonal_owner, (4, CELLS)),
        in_hbm(merid_state, flat_shape),
        in_hbm(merid_courant, (LANES, CELLS)),
        in_hbm(mixing, (LANES, 32)),
    )
    out_z, out_m, out_c = pl.pallas_call(
        write_out,
        out_shape=(
            pltpu.HBM(flat_shape, F32),
            pltpu.HBM(flat_shape, F32),
            pltpu.HBM((4 * GLON_DEV, LANES), F32),
        ),
        in_specs=[vmem, vmem, vmem],
        out_specs=(hbm, hbm, hbm),
        scratch_shapes=[pltpu.SemaphoreType.DMA((3,))],
        compiler_params=pltpu.CompilerParams(vmem_limit_bytes=1024 * 1024),
    )(out_z, out_m, out_c)
    return (
        out_z.reshape(zonal_state.shape),
        out_m.reshape(merid_state.shape),
        out_c.reshape(GLON_DEV, 4, LANES),
    )


def solution(mesh):
    counts = (mesh.shape["lon"], mesh.shape["lat"])
    return jax.shard_map(
        functools.partial(shards, counts),
        mesh=mesh,
        in_specs=(
            P(None, None, None, "lat", "lon"),
            P(None, "lat", "lon"),
            P("lat"),
            P("lat", "lon"),
            P(None, None, None, "lon", "lat"),
            P(None, "lon", "lat"),
            P(),
        ),
        out_specs=(
            P(None, None, None, "lat", "lon"),
            P(None, None, None, "lon", "lat"),
            P("lon", "lat", None),
        ),
        check_vma=False,
    )
```

```python
import functools

import jax
import jax.numpy as jnp
from jax import lax
from jax.experimental import pallas as pl
from jax.experimental.pallas import tpu as pltpu
from jax.sharding import PartitionSpec as P

SUB = 4
OFF = 8
CELLS = 128
LANES = 128
ROWS = 152
WIN = 16
SROWS = 32
PROWS = 272
PBASE = 136
GLON_DEV = 4
FAR = (0, 2, 3)
MESH = pl.DeviceIdType.MESH
F32 = jnp.float32
BF16 = jnp.bfloat16


def two_parts(value):
    high = value.astype(BF16)
    low = (value - high.astype(F32)).astype(BF16)
    return high, low


def advance(src, dst, courant, weights, items, rows, chunk):
    group = max(1, CELLS // rows)
    for first_item in range(0, len(items), group):
        some = items[first_item : first_item + group]
        parts = [
            jnp.concatenate(two_parts(src(item, w, OFF, rows)), axis=1)
            for item in some
            for w in range(3)
        ]
        product = jnp.dot(
            jnp.concatenate(parts, axis=0), weights[...], preferred_element_type=F32
        )
        for n, item in enumerate(some):
            for at in range(0, rows, chunk):
                half = 0.5 * courant(item, at, chunk)
                ahead_share, behind_share = 0.3 - half, 0.3 + half
                here = [src(item, w, OFF + at, chunk) for w in range(3)]
                for w, (one, other) in enumerate(((0, 1), (0, 2), (1, 2))):
                    spot = (n * 3 + w) * rows + at
                    mixed = (
                        product[spot : spot + chunk, 0:LANES] + product[spot : spot + chunk, LANES:]
                    )
                    along = ahead_share * src(item, w, OFF + at + 1, chunk) + behind_share * src(
                        item, w, OFF + at - 1, chunk
                    )
                    dst(item, w, OFF + at, chunk, mixed + along + 0.1 * (here[one] + here[other]))


def relays_of(lon_count):
    tail_from, half_turn = lon_count // 4 - 1, lon_count // 2
    first_ones = (half_turn + tail_from, tail_from, half_turn - 1, lon_count - 1, half_turn)
    relays = {dev: [] for dev in first_ones}
    for first, last in ((tail_from, half_turn - 1), (half_turn + tail_from, lon_count - 1)):
        for dev in range(first + 1, last):
            relays[first if dev <= first + 2 else last].append(dev)
    for dev in range(half_turn + 1, half_turn + tail_from):
        relays[dev] = []
    return relays


def kernel(
    counts,
    zlen_ref,
    zs,
    zc,
    owner_ref,
    ms,
    mc,
    mix_ref,
    out_z,
    out_m,
    out_c,
    raw,
    rawc,
    owner,
    mix,
    zlen,
    first,
    state,
    other_state,
    weights,
    strips,
    other_strips,
    scour,
    back,
    edges,
    halos,
    tails,
    gathered,
    gathered_0,
    heads,
    part,
    part_in,
    load_sem,
    send_sem,
    recv_sem,
    far_send,
    far_recv,
    entry_sem,
):
    lon_count, lat_count = counts
    half_turn = lon_count // 2
    tail_from = lon_count // 4 - 1
    tail_devs = list(range(tail_from, lon_count))
    relays = relays_of(lon_count)
    me, lat = lax.axis_index("lon"), lax.axis_index("lat")
    left = lax.rem(me + lon_count - 1, lon_count)
    right = lax.rem(me + 1, lon_count)
    across = lax.rem(me + half_turn, lon_count)
    at_south, at_north = lat == 0, lat == lat_count - 1
    south = {"lon": jnp.where(at_south, across, me), "lat": jnp.where(at_south, lat, lat - 1)}
    north = {"lon": jnp.where(at_north, across, me), "lat": jnp.where(at_north, lat, lat + 1)}
    west, east = {"lon": left, "lat": lat}, {"lon": right, "lat": lat}
    root = {"lon": 0 * me, "lat": lat}
    is_root, is_tail, is_half = me == 0, me >= tail_from, me == half_turn

    loads = []
    for f, (s_ref, c_ref) in enumerate(((zs, zc), (ms, mc))):
        loads.append(pltpu.make_async_copy(s_ref, raw.at[f], load_sem.at[f, 0]))
        loads.append(pltpu.make_async_copy(c_ref, rawc.at[f], load_sem.at[f, 1]))
    loads.append(pltpu.make_async_copy(mix_ref, mix, load_sem.at[2, 0]))
    loads.append(pltpu.make_async_copy(owner_ref, owner, load_sem.at[2, 1]))
    loads.append(pltpu.make_async_copy(zlen_ref, zlen, load_sem.at[3, 0]))
    for load in loads:
        load.start()

    place = lax.rem(me, half_turn)
    is_late, is_early = place >= half_turn // 2, place == 0
    in_middle = (lat == lat_count // 2 - 1) | (lat == lat_count // 2)
    is_mid = (place == tail_from) | (in_middle & jnp.logical_not(is_late | is_early))
    answers = is_late & (lat == lat_count // 2 - 1)
    asks = is_late & (lat == lat_count // 2)

    barrier = pltpu.get_barrier_semaphore()
    for peer in (west, east, south):
        pl.semaphore_signal(barrier, inc=1, device_id=peer, device_id_type=MESH)

    @pl.when(jnp.logical_not(answers))
    def _():
        pl.semaphore_signal(barrier, inc=1, device_id=north, device_id_type=MESH)

    def sector(dev):
        return {"lon": 0 * me + dev, "lat": lat}

    child_count = 0 * me
    for relay, children in relays.items():
        child_count = child_count + jnp.where(me == relay, len(children), 0)

        @pl.when(me == relay)
        def _():
            pl.semaphore_signal(barrier, inc=1, device_id=root, device_id_type=MESH)

        if children:

            @pl.when((me >= children[0]) & (me <= children[-1]))
            def _(relay=relay):
                pl.semaphore_signal(
                    barrier, inc=1, device_id=sector(relay), device_id_type=MESH
                )

    zonal_first = jnp.logical_not(is_root)
    peers = 4 - jnp.where(asks, 1, 0) + jnp.where(is_tail, 1, 0) + child_count + jnp.where(is_root, len(relays), 0)

    @pl.when(is_root)
    def _():
        for dev in tail_devs:
            pl.semaphore_signal(
                barrier, inc=1, device_id={"lon": 0 * me + dev, "lat": lat}, device_id_type=MESH
            )

    def turn_in(f, channels):
        if channels[0] != 1:
            loads[2 * f].wait()
            loads[2 * f + 1].wait()
        for r in channels:
            for w in range(3):
                turned = raw[f, pl.ds(w * 4 + r, LANES, stride=12), :].T
                first[4 * f + r, w, OFF : OFF + CELLS, :] = turned
                state[4 * f + r, w, OFF : OFF + CELLS, :] = turned
            c_now = rawc[f, pl.ds(r, 32, stride=4), :]
            first[4 * f + r, 3, OFF : OFF + CELLS, :] = jnp.concatenate([c_now] * 4, axis=0).T
        for r in channels:
            for p in range(4):
                edges[f, 0, r, 4 * p : 4 * p + 4, :] = first[4 * f + r, p, OFF : OFF + SUB, :]
                edges[f, 1, r, 4 * p : 4 * p + 4, :] = first[
                    4 * f + r, p, OFF + CELLS - SUB : OFF + CELLS, :
                ]

    with jax.named_scope("turn_z"):
        turn_in(0, (2, 3, 0))
        loads[6].wait()
        ends = [jnp.clip(zlen[r] - me * CELLS, 0, CELLS + SUB) for r in range(4)]
        quarter = lax.broadcasted_iota(jnp.int32, (8, LANES), 0)
        for r in FAR:
            cell = ends[r] - SUB + quarter
            own = (cell >= 0) & (cell < CELLS)
            for p in range(4):
                found = jnp.where(own, first[r, p, pl.ds(OFF + ends[r] - SUB, 8), :], 0.0)
                tails[r, 4 * p : 4 * p + 4, :] = found[0:SUB]
        turn_in(0, (1,))

    def remote(src, dst, s_sem, r_sem, peer):
        return pltpu.make_async_remote_copy(
            src_ref=src,
            dst_ref=dst,
            send_sem=s_sem,
            recv_sem=r_sem,
            device_id=peer,
            device_id_type=MESH,
        )

    slot = jnp.maximum(me - tail_from, 0)
    tail_copy = remote(
        tails.at[2:4], gathered.at[slot], far_send.at[0], far_recv.at[slot], root
    )
    tail_0_copy = remote(
        tails.at[0], gathered_0, far_send.at[1], recv_sem.at[7], root
    )
    head_copies = [
        remote(
            edges.at[0, 0, 2:4], heads.at[2:4], far_send.at[2 + n], recv_sem.at[8], sector(relay)
        )
        for n, relay in enumerate(relays)
    ]
    head_0_copy = remote(
        edges.at[0, 0, 0], heads.at[0], far_send.at[1], recv_sem.at[9], sector(half_turn)
    )
    passed_on = {
        relay: [
            remote(heads.at[2:4], heads.at[2:4], far_send.at[2 + n], recv_sem.at[8], sector(dev))
            for n, dev in enumerate(children)
        ]
        for relay, children in relays.items()
    }

    south_side, north_side = jnp.where(at_south, 0, 1), jnp.where(at_north, 1, 0)
    near = [
        remote(edges.at[0, 0], halos.at[0, 1], send_sem.at[0], recv_sem.at[1], west),
        remote(edges.at[0, 1], halos.at[0, 0], send_sem.at[1], recv_sem.at[0], east),
        remote(
            edges.at[1, 0],
            halos.at[1, south_side],
            send_sem.at[2],
            recv_sem.at[2 + south_side],
            south,
        ),
        remote(
            edges.at[1, 1],
            halos.at[1, north_side],
            send_sem.at[3],
            recv_sem.at[2 + north_side],
            north,
        ),
    ]
    def entered(first_send=None):
        with jax.named_scope("barrier"):
            pl.semaphore_wait(barrier, peers)

        if first_send is not None:
            first_send()

        @pl.when(answers)
        def _():
            pl.semaphore_signal(entry_sem, inc=1, device_id=north, device_id_type=MESH)

        @pl.when(is_tail)
        def _():
            tail_copy.start()

        @pl.when(is_half)
        def _():
            tail_0_copy.start()

        for copy in near[:2]:
            copy.start()

        @pl.when(is_root)
        def _():
            for copy in head_copies[3:]:
                copy.start()
            head_0_copy.start()

    def then_send():
        @pl.when(is_root)
        def _():
            for copy in head_copies[:3]:
                copy.start()

        near[3].start()

        @pl.when(jnp.logical_not(asks))
        def _():
            near[2].start()

    @pl.when(jnp.logical_not(is_early | is_mid))
    def _():
        entered()

    with jax.named_scope("turn_m"):
        turn_in(1, (0, 1, 2, 3))

    loads[4].wait()
    loads[5].wait()
    spread = jnp.concatenate([mix[...]] * 4, axis=1)
    row_at = lax.broadcasted_iota(jnp.int32, (LANES, LANES), 0)
    lane_at = lax.broadcasted_iota(jnp.int32, (LANES, LANES), 1)
    spread = jnp.where(row_at // 32 == lane_at // 32, spread, 0.0)
    spread = spread + jnp.where(row_at == lane_at, 0.2, 0.0)
    high, low = two_parts(spread.T)
    for row in (0, LANES):
        weights[row : row + LANES, 0:LANES] = high
        weights[row : row + LANES, LANES:] = low

    def one_way(there, back, courant, items, rows, chunk):
        def src(item, w, at, size):
            return there[item, w, pl.ds(at, size), :]

        def dst(item, w, at, size, value):
            back[item, w, pl.ds(at, size), :] = value

        advance(src, dst, courant, weights, items, rows, chunk)

    def two_steps(there, back, courant, items, rows, chunk):
        one_way(there, back, courant, items, rows, chunk)
        one_way(back, there, courant, items, rows, chunk)

    def interior(f):
        items = [4 * f + r for r in range(4)]

        def courant(ch, at, size):
            return first[ch, 3, pl.ds(OFF + at, size), :]

        def step(t, carry):
            two_steps(state, other_state, courant, items, CELLS, 16)
            return carry

        lax.fori_loop(0, SUB // 2, step, 0)

    def arrived(f, side):
        pltpu.make_async_copy(
            halos.at[f, side], halos.at[f, side], recv_sem.at[2 * f + side]
        ).wait()

    def strip_steps(count):
        def step(t, carry):
            two_steps(
                strips,
                other_strips,
                lambda n, at, size: scour[n, pl.ds(at, size), :],
                list(range(count)),
                WIN,
                16,
            )
            return carry

        lax.fori_loop(0, SUB // 2, step, 0)

    def fill(n, ch, start):
        for w in range(3):
            strips[n, w, OFF : OFF + WIN, :] = first[ch, w, pl.ds(start, WIN), :]
        scour[n, :, :] = first[ch, 3, pl.ds(start, WIN), :]

    left_row, right_row = OFF - SUB, OFF + CELLS
    left_start, right_start = OFF - SUB, OFF + CELLS + SUB - WIN
    near_columns = me * GLON_DEV - 1 + lax.broadcasted_iota(jnp.int32, (8, CELLS), 0)
    column = lax.broadcasted_iota(jnp.int32, (CELLS, LANES), 0)
    scale = GLON_DEV / (3.0 * CELLS)
    back_copy = remote(part.at[4], part_in.at[1], send_sem.at[4], recv_sem.at[5], west)
    on_copy = remote(part.at[5], part_in.at[0], send_sem.at[5], recv_sem.at[4], east)
    is_last = me == lon_count - 1

    def merid_end():
        with jax.named_scope("merid_wait"):
            arrived(1, 0)
            arrived(1, 1)
        for side, turned, row in ((0, at_south, left_row), (1, at_north, right_row)):
            for r in range(4):
                for p in range(4):
                    plain = halos[1, side, r, 4 * p : 4 * p + 4, :]
                    q = p if p == 3 else 2 - p
                    mirrored = jnp.concatenate(
                        [halos[1, side, r, 4 * q + 3 - j : 4 * q + 4 - j, :] for j in range(SUB)],
                        axis=0,
                    )
                    if p == 3:
                        mirrored = -mirrored
                    first[4 + r, p, row : row + SUB, :] = jnp.where(turned, mirrored, plain)
        for r in range(4):
            fill(r, 4 + r, left_start)
            fill(4 + r, 4 + r, right_start)
        with jax.named_scope("merid_strips"):
            strip_steps(8)
        for r in range(4):
            for w in range(3):
                kept = strips[r, w, OFF + 4 : OFF + 8, :]
                state[4 + r, w, OFF : OFF + SUB, :] = kept
                kept = strips[4 + r, w, OFF + 8 : OFF + 12, :]
                state[4 + r, w, OFF + CELLS - SUB : OFF + CELLS, :] = kept
        for r in range(4):
            for w in range(3):
                out_m[pl.ds(w * 4 + r, LANES, stride=12), :] = state[
                    4 + r, w, OFF : OFF + CELLS, :
                ].T

    def shares(r, change):
        high, low = two_parts(change * scale)
        mine = (jnp.broadcast_to(owner[r : r + 1, :], (8, CELLS)) == near_columns).astype(BF16)
        return jnp.dot(
            jnp.concatenate([mine, mine], axis=1),
            jnp.concatenate([high, low], axis=0),
            preferred_element_type=F32,
        )

    def right_strips(at):
        for r in range(4):
            for p in range(4):
                first[r, p, right_row : right_row + SUB, :] = halos[0, 1, r, 4 * p : 4 * p + 4, :]
        for r in range(4):
            fill(at + r, r, right_start)

    def right_kept(at):
        for r in range(4):
            for w in range(3):
                kept = strips[at + r, w, OFF + 8 : OFF + 12, :]
                state[r, w, OFF + CELLS - SUB : OFF + CELLS, :] = kept

    passing = {relay: copies for relay, copies in passed_on.items() if copies}
    is_relay = functools.reduce(jnp.logical_or, [me == relay for relay in passing])

    def heads_arrived():
        pltpu.make_async_copy(heads.at[2:4], heads.at[2:4], recv_sem.at[8]).wait()

    def pass_on():
        with jax.named_scope("pass_on"):
            for relay, copies in passing.items():

                @pl.when(me == relay)
                def _(copies=copies):
                    heads_arrived()
                    for copy in copies:
                        copy.start()

    def left_kept(at):
        for r in range(4):
            for w in range(3):
                kept = strips[at + r, w, OFF + 4 : OFF + 8, :]
                state[r, w, OFF : OFF + SUB, :] = kept

    def early_part():
        arrived(0, 1)
        with jax.named_scope("early_part"):
            right_strips(0)
            strip_steps(4)
            right_kept(0)
            for r in range(4):
                change = None
                for w in range(3):
                    value = (
                        state[r, w, OFF : OFF + CELLS, :] - first[r, w, OFF : OFF + CELLS, :]
                    )
                    change = value if change is None else change + value
                change = jnp.where(column >= SUB, change, 0.0)
                part[5, r : r + 1, :] = shares(r, change)[5:6]
            on_copy.start()

    def zonal_end(first_wait=True):
        if first_wait:
            with jax.named_scope("right_wait"):
                arrived(0, 1)

        with jax.named_scope("left_wait"):
            arrived(0, 0)
        for r in range(4):
            for p in range(4):
                first[r, p, left_row : left_row + SUB, :] = halos[0, 0, r, 4 * p : 4 * p + 4, :]

        def edge_strips():
            right_strips(0)
            for r in range(4):
                fill(4 + r, r, left_start)

        def edges_kept():
            right_kept(0)
            left_kept(4)

        def far_arrived():
            with jax.named_scope("far_wait"):

                @pl.when(jnp.logical_not(is_relay))
                def _():
                    heads_arrived()

                @pl.when(is_half)
                def _():
                    pltpu.make_async_copy(heads.at[0], heads.at[0], recv_sem.at[9]).wait()

        def far_strips(at):
            for n, r in enumerate(FAR):
                fill(at + n, r, ends[r])
                for w in range(3):
                    strips[at + n, w, OFF + 8 : OFF + 12, :] = heads[r, 4 * w : 4 * w + 4, :]
                scour[at + n, 8:12, :] = heads[r, 12:16, :]

        def far_kept(at):
            for n in range(len(FAR)):
                for w in range(3):
                    back[n, w, PBASE : PBASE + WIN, :] = strips[at + n, w, OFF : OFF + WIN, :]

        in_one = me == half_turn - 1

        @pl.when(in_one)
        def _():
            edge_strips()
            far_strips(8)
            with jax.named_scope("zonal_strips"):
                strip_steps(11)
            edges_kept()
            far_kept(8)

        @pl.when(jnp.logical_not(in_one | is_root))
        def _():
            edge_strips()
            with jax.named_scope("zonal_strips"):
                strip_steps(8)
            edges_kept()

        @pl.when(is_tail & jnp.logical_not(in_one))
        def _():
            far_arrived()
            far_strips(0)
            with jax.named_scope("far_strips"):
                strip_steps(3)
            far_kept(0)

        @pl.when(is_root)
        def _():
            with jax.named_scope("far_wait"):
                for n in range(len(tail_devs)):
                    pltpu.make_async_copy(gathered.at[n], gathered.at[n], far_recv.at[n]).wait()
                pltpu.make_async_copy(gathered_0, gathered_0, recv_sem.at[7]).wait()
            for r in FAR:
                if r == 0:
                    tail_cells = gathered_0[...]
                else:
                    tail_cells = gathered[0, r - 2]
                    for n in range(1, len(tail_devs)):
                        tail_cells = tail_cells + gathered[n, r - 2]
                for p in range(4):
                    first[r, p, left_row : left_row + SUB, :] = tail_cells[4 * p : 4 * p + 4]
            for r in range(4):
                fill(r, r, left_start)
            with jax.named_scope("far_strips"):
                strip_steps(4)
            left_kept(0)

        for r in range(4):
            change = None
            for w in range(3):
                value = state[r, w, OFF : OFF + CELLS, :]
                before = first[r, w, OFF : OFF + CELLS, :]
                if r in FAR:
                    n = FAR.index(r)
                    cut = ends[r]
                    strip = back[n, w, pl.ds(PBASE + 8 - cut, CELLS), :]
                    value = jnp.where(column >= cut - SUB, strip, value)
                    value = jnp.where(column < cut, value, before)
                    state[r, w, OFF : OFF + CELLS, :] = value
                change = value - before if change is None else change + (value - before)
            part[r, :, :] = shares(r, change)

        @pl.when(jnp.logical_not(is_root))
        def _():
            for r in range(4):
                part[4, r : r + 1, :] = part[r, 0:1, :]
            back_copy.start()

        @pl.when(jnp.logical_not(is_root | is_last))
        def _():
            for r in range(4):
                part[5, r : r + 1, :] = part[r, 5:6, :]
            on_copy.start()

    @pl.when(jnp.logical_not(is_early | is_mid))
    def _():
        then_send()

    @pl.when(is_late)
    def _():
        with jax.named_scope("interior_z"):
            interior(0)
        pass_on()

        @pl.when(asks)
        def _():
            with jax.named_scope("answer_wait"):
                pl.semaphore_wait(entry_sem, 1)
            near[2].start()

        zonal_end()
        with jax.named_scope("interior_m"):
            interior(1)
        merid_end()

    @pl.when(jnp.logical_not(is_late))
    def _():
        with jax.named_scope("interior_m"):
            interior(1)

        @pl.when(is_mid | is_early)
        def _():
            entered(then_send)

        with jax.named_scope("interior_z"):
            interior(0)

        @pl.when(is_root)
        def _():
            early_part()

        @pl.when(is_early | is_mid)
        def _():
            pass_on()

        @pl.when(jnp.logical_not(is_root))
        def _():
            with jax.named_scope("right_wait"):
                arrived(0, 1)

        @pl.when(jnp.logical_not(zonal_first))
        def _():
            merid_end()

        @pl.when(jnp.logical_not(is_early | is_mid))
        def _():
            pass_on()

        zonal_end(False)

        @pl.when(zonal_first)
        def _():
            merid_end()

    for r in range(4):
        for w in range(3):
            out_z[pl.ds(w * 4 + r, LANES, stride=12), :] = state[r, w, OFF : OFF + CELLS, :].T

    with jax.named_scope("part_wait"):

        @pl.when(is_root)
        def _():
            part_in[0, :, :] = jnp.zeros((8, LANES), F32)

        @pl.when(is_last)
        def _():
            part_in[1, :, :] = jnp.zeros((8, LANES), F32)

        @pl.when(jnp.logical_not(is_last))
        def _():
            back_copy.wait_recv()

        @pl.when(jnp.logical_not(is_root))
        def _():
            on_copy.wait_recv()

    for r in range(4):
        for g in range(GLON_DEV):
            value = part[r, g + 1 : g + 2, :]
            if g == 0:
                value = value + part_in[0, r : r + 1, :]
            if g == GLON_DEV - 1:
                value = value + part_in[1, r : r + 1, :]
            out_c[4 * g + r : 4 * g + r + 1, :] = value

    for copy in near:
        copy.wait_send()

    @pl.when(jnp.logical_not(is_root))
    def _():
        back_copy.wait_send()

    @pl.when(jnp.logical_not(is_last))
    def _():
        on_copy.wait_send()

    @pl.when(is_tail)
    def _():
        tail_copy.wait_send()

    @pl.when(is_half)
    def _():
        tail_0_copy.wait_send()

    for relay, copies in passing.items():

        @pl.when(me == relay)
        def _(copies=copies):
            for copy in copies:
                copy.wait_send()

    @pl.when(is_root)
    def _():
        head_0_copy.wait_send()
        for copy in head_copies:
            copy.wait_send()


def write_out(z, m, c, out_z, out_m, out_c, sem):
    copies = [
        pltpu.make_async_copy(src, dst, sem.at[n])
        for n, (src, dst) in enumerate(((z, out_z), (m, out_m), (c, out_c)))
    ]
    for copy in copies:
        copy.start()
    for copy in copies:
        copy.wait()


def shards(
    counts, zonal_state, zonal_courant, zonal_length, zonal_owner, merid_state, merid_courant, mixing
):
    tail_count = counts[0] - (counts[0] // 4 - 1)
    relays = relays_of(counts[0])
    hbm = pl.BlockSpec(memory_space=pltpu.HBM)
    vmem = pl.BlockSpec(memory_space=pltpu.VMEM)
    flat_shape = (LANES * 12, CELLS)

    def in_hbm(array, shape):
        return pltpu.with_memory_space_constraint(array.reshape(shape), pltpu.HBM)

    out_z, out_m, out_c = pl.pallas_call(
        functools.partial(kernel, counts),
        out_shape=(
            pltpu.VMEM(flat_shape, F32),
            pltpu.VMEM(flat_shape, F32),
            pltpu.VMEM((4 * GLON_DEV, LANES), F32),
        ),
        in_specs=[hbm, hbm, hbm, hbm, hbm, hbm, hbm],
        out_specs=(vmem, vmem, vmem),
        scratch_shapes=[
            pltpu.VMEM((2, *flat_shape), F32),
            pltpu.VMEM((2, LANES, CELLS), F32),
            pltpu.VMEM((4, CELLS), jnp.int32),
            pltpu.VMEM((LANES, 32), F32),
            pltpu.SMEM((4,), jnp.int32),
            pltpu.VMEM((8, 4, ROWS, LANES), F32),
            pltpu.VMEM((8, 3, ROWS, LANES), F32),
            pltpu.VMEM((8, 3, ROWS, LANES), F32),
            pltpu.VMEM((2 * LANES, 2 * LANES), BF16),
            pltpu.VMEM((12, 3, SROWS, LANES), F32),
            pltpu.VMEM((12, 3, SROWS, LANES), F32),
            pltpu.VMEM((12, WIN, LANES), F32),
            pltpu.VMEM((3, 3, PROWS, LANES), F32),
            pltpu.VMEM((2, 2, 4, 16, LANES), F32),
            pltpu.VMEM((2, 2, 4, 16, LANES), F32),
            pltpu.VMEM((4, 16, LANES), F32),
            pltpu.VMEM((tail_count, 2, 16, LANES), F32),
            pltpu.VMEM((16, LANES), F32),
            pltpu.VMEM((4, 16, LANES), F32),
            pltpu.VMEM((6, 8, LANES), F32),
            pltpu.VMEM((2, 8, LANES), F32),
            pltpu.SemaphoreType.DMA((4, 2)),
            pltpu.SemaphoreType.DMA((6,)),
            pltpu.SemaphoreType.DMA((10,)),
            pltpu.SemaphoreType.DMA((2 + max(map(len, (relays, *relays.values()))),)),
            pltpu.SemaphoreType.DMA((tail_count,)),
            pltpu.SemaphoreType.REGULAR,
        ],
        compiler_params=pltpu.CompilerParams(
            collective_id=0, has_side_effects=True, vmem_limit_bytes=32 * 1024 * 1024
        ),
    )(
        in_hbm(zonal_length, (4,)),
        in_hbm(zonal_state, flat_shape),
        in_hbm(zonal_courant, (LANES, CELLS)),
        in_hbm(zonal_owner, (4, CELLS)),
        in_hbm(merid_state, flat_shape),
        in_hbm(merid_courant, (LANES, CELLS)),
        in_hbm(mixing, (LANES, 32)),
    )
    out_z, out_m, out_c = pl.pallas_call(
        write_out,
        out_shape=(
            pltpu.HBM(flat_shape, F32),
            pltpu.HBM(flat_shape, F32),
            pltpu.HBM((4 * GLON_DEV, LANES), F32),
        ),
        in_specs=[vmem, vmem, vmem],
        out_specs=(hbm, hbm, hbm),
        scratch_shapes=[pltpu.SemaphoreType.DMA((3,))],
        compiler_params=pltpu.CompilerParams(vmem_limit_bytes=1024 * 1024),
    )(out_z, out_m, out_c)
    return (
        out_z.reshape(zonal_state.shape),
        out_m.reshape(merid_state.shape),
        out_c.reshape(GLON_DEV, 4, LANES),
    )


def solution(mesh):
    counts = (mesh.shape["lon"], mesh.shape["lat"])
    return jax.shard_map(
        functools.partial(shards, counts),
        mesh=mesh,
        in_specs=(
            P(None, None, None, "lat", "lon"),
            P(None, "lat", "lon"),
            P("lat"),
            P("lat", "lon"),
            P(None, None, None, "lon", "lat"),
            P(None, "lon", "lat"),
            P(),
        ),
        out_specs=(
            P(None, None, None, "lat", "lon"),
            P(None, None, None, "lon", "lat"),
            P("lon", "lat", None),
        ),
        check_vma=False,
    )
```

```python
import functools

import jax
import jax.numpy as jnp
from jax import lax
from jax.experimental import pallas as pl
from jax.experimental.pallas import tpu as pltpu
from jax.sharding import PartitionSpec as P

SUB = 4
OFF = 8
CELLS = 128
LANES = 128
ROWS = 152
WIN = 16
SROWS = 32
PROWS = 272
PBASE = 136
GLON_DEV = 4
FAR = (0, 2, 3)
MESH = pl.DeviceIdType.MESH
F32 = jnp.float32
BF16 = jnp.bfloat16


def two_parts(value):
    high = value.astype(BF16)
    low = (value - high.astype(F32)).astype(BF16)
    return high, low


def advance(src, dst, courant, weights, items, rows, chunk):
    group = max(1, CELLS // rows)
    for first_item in range(0, len(items), group):
        some = items[first_item : first_item + group]
        parts = [
            jnp.concatenate(two_parts(src(item, w, OFF, rows)), axis=1)
            for item in some
            for w in range(3)
        ]
        product = jnp.dot(
            jnp.concatenate(parts, axis=0), weights[...], preferred_element_type=F32
        )
        for n, item in enumerate(some):
            for at in range(0, rows, chunk):
                half = 0.5 * courant(item, at, chunk)
                ahead_share, behind_share = 0.3 - half, 0.3 + half
                here = [src(item, w, OFF + at, chunk) for w in range(3)]
                for w, (one, other) in enumerate(((0, 1), (0, 2), (1, 2))):
                    spot = (n * 3 + w) * rows + at
                    mixed = (
                        product[spot : spot + chunk, 0:LANES] + product[spot : spot + chunk, LANES:]
                    )
                    along = ahead_share * src(item, w, OFF + at + 1, chunk) + behind_share * src(
                        item, w, OFF + at - 1, chunk
                    )
                    dst(item, w, OFF + at, chunk, mixed + along + 0.1 * (here[one] + here[other]))


def relays_of(lon_count):
    tail_from, half_turn = lon_count // 4 - 1, lon_count // 2
    first_ones = (half_turn + tail_from, tail_from, half_turn - 1, lon_count - 1, half_turn)
    relays = {dev: [] for dev in first_ones}
    for first, last in ((tail_from, half_turn - 1), (half_turn + tail_from, lon_count - 1)):
        for dev in range(first + 1, last):
            relays[first if dev <= first + 2 else last].append(dev)
    for dev in range(half_turn + 1, half_turn + tail_from):
        relays[dev] = []
    return relays


def kernel(
    counts,
    zlen_ref,
    zs,
    zc,
    owner_ref,
    ms,
    mc,
    mix_ref,
    out_z,
    out_m,
    out_c,
    raw,
    rawc,
    owner,
    mix,
    zlen,
    first,
    state,
    other_state,
    weights,
    strips,
    other_strips,
    scour,
    back,
    owners,
    edges,
    halos,
    tails,
    gathered,
    gathered_0,
    heads,
    part,
    part_in,
    load_sem,
    send_sem,
    recv_sem,
    far_send,
    far_recv,
    entry_sem,
):
    lon_count, lat_count = counts
    half_turn = lon_count // 2
    tail_from = lon_count // 4 - 1
    tail_devs = list(range(tail_from, lon_count))
    relays = relays_of(lon_count)
    me, lat = lax.axis_index("lon"), lax.axis_index("lat")
    left = lax.rem(me + lon_count - 1, lon_count)
    right = lax.rem(me + 1, lon_count)
    across = lax.rem(me + half_turn, lon_count)
    at_south, at_north = lat == 0, lat == lat_count - 1
    south = {"lon": jnp.where(at_south, across, me), "lat": jnp.where(at_south, lat, lat - 1)}
    north = {"lon": jnp.where(at_north, across, me), "lat": jnp.where(at_north, lat, lat + 1)}
    west, east = {"lon": left, "lat": lat}, {"lon": right, "lat": lat}
    root = {"lon": 0 * me, "lat": lat}
    is_root, is_tail, is_half = me == 0, me >= tail_from, me == half_turn

    loads = []
    for f, (s_ref, c_ref) in enumerate(((zs, zc), (ms, mc))):
        loads.append(pltpu.make_async_copy(s_ref, raw.at[f], load_sem.at[f, 0]))
        loads.append(pltpu.make_async_copy(c_ref, rawc.at[f], load_sem.at[f, 1]))
    loads.append(pltpu.make_async_copy(mix_ref, mix, load_sem.at[2, 0]))
    loads.append(pltpu.make_async_copy(owner_ref, owner, load_sem.at[2, 1]))
    loads.append(pltpu.make_async_copy(zlen_ref, zlen, load_sem.at[3, 0]))
    for load in loads:
        load.start()

    place = lax.rem(me, half_turn)
    is_late, is_early = place >= half_turn // 2, place == 0
    in_middle = (lat == lat_count // 2 - 1) | (lat == lat_count // 2)
    is_mid = (place == tail_from) | (in_middle & jnp.logical_not(is_late | is_early))
    answers = is_late & (lat == lat_count // 2 - 1)
    asks = is_late & (lat == lat_count // 2)

    barrier = pltpu.get_barrier_semaphore()
    for peer in (west, east, south):
        pl.semaphore_signal(barrier, inc=1, device_id=peer, device_id_type=MESH)

    @pl.when(jnp.logical_not(answers))
    def _():
        pl.semaphore_signal(barrier, inc=1, device_id=north, device_id_type=MESH)

    def sector(dev):
        return {"lon": 0 * me + dev, "lat": lat}

    child_count = 0 * me
    for relay, children in relays.items():
        child_count = child_count + jnp.where(me == relay, len(children), 0)

        @pl.when(me == relay)
        def _():
            pl.semaphore_signal(barrier, inc=1, device_id=root, device_id_type=MESH)

        if children:

            @pl.when((me >= children[0]) & (me <= children[-1]))
            def _(relay=relay):
                pl.semaphore_signal(
                    barrier, inc=1, device_id=sector(relay), device_id_type=MESH
                )

    zonal_first = jnp.logical_not(is_root)
    peers = 4 - jnp.where(asks, 1, 0) + jnp.where(is_tail, 1, 0) + child_count + jnp.where(is_root, len(relays), 0)

    @pl.when(is_root)
    def _():
        for dev in tail_devs:
            pl.semaphore_signal(
                barrier, inc=1, device_id={"lon": 0 * me + dev, "lat": lat}, device_id_type=MESH
            )

    def turn_in(f, channels):
        if channels[0] != 1:
            loads[2 * f].wait()
            loads[2 * f + 1].wait()
        for r in channels:
            for w in range(3):
                turned = raw[f, pl.ds(w * 4 + r, LANES, stride=12), :].T
                first[4 * f + r, w, OFF : OFF + CELLS, :] = turned
                state[4 * f + r, w, OFF : OFF + CELLS, :] = turned
            c_now = rawc[f, pl.ds(r, 32, stride=4), :]
            first[4 * f + r, 3, OFF : OFF + CELLS, :] = jnp.concatenate([c_now] * 4, axis=0).T
        for r in channels:
            for p in range(4):
                edges[f, 0, r, 4 * p : 4 * p + 4, :] = first[4 * f + r, p, OFF : OFF + SUB, :]
                edges[f, 1, r, 4 * p : 4 * p + 4, :] = first[
                    4 * f + r, p, OFF + CELLS - SUB : OFF + CELLS, :
                ]

    with jax.named_scope("turn_z"):
        turn_in(0, (2, 3, 0))
        loads[6].wait()
        ends = [jnp.clip(zlen[r] - me * CELLS, 0, CELLS + SUB) for r in range(4)]
        quarter = lax.broadcasted_iota(jnp.int32, (8, LANES), 0)
        for r in FAR:
            cell = ends[r] - SUB + quarter
            own = (cell >= 0) & (cell < CELLS)
            for p in range(4):
                found = jnp.where(own, first[r, p, pl.ds(OFF + ends[r] - SUB, 8), :], 0.0)
                tails[r, 4 * p : 4 * p + 4, :] = found[0:SUB]
        turn_in(0, (1,))

    def remote(src, dst, s_sem, r_sem, peer):
        return pltpu.make_async_remote_copy(
            src_ref=src,
            dst_ref=dst,
            send_sem=s_sem,
            recv_sem=r_sem,
            device_id=peer,
            device_id_type=MESH,
        )

    slot = jnp.maximum(me - tail_from, 0)
    tail_copy = remote(
        tails.at[2:4], gathered.at[slot], far_send.at[0], far_recv.at[slot], root
    )
    tail_0_copy = remote(
        tails.at[0], gathered_0, far_send.at[1], recv_sem.at[7], root
    )
    head_copies = [
        remote(
            edges.at[0, 0, 2:4], heads.at[2:4], far_send.at[2 + n], recv_sem.at[8], sector(relay)
        )
        for n, relay in enumerate(relays)
    ]
    head_0_copy = remote(
        edges.at[0, 0, 0], heads.at[0], far_send.at[1], recv_sem.at[9], sector(half_turn)
    )
    passed_on = {
        relay: [
            remote(heads.at[2:4], heads.at[2:4], far_send.at[2 + n], recv_sem.at[8], sector(dev))
            for n, dev in enumerate(children)
        ]
        for relay, children in relays.items()
    }

    south_side, north_side = jnp.where(at_south, 0, 1), jnp.where(at_north, 1, 0)
    near = [
        remote(edges.at[0, 0], halos.at[0, 1], send_sem.at[0], recv_sem.at[1], west),
        remote(edges.at[0, 1], halos.at[0, 0], send_sem.at[1], recv_sem.at[0], east),
        remote(
            edges.at[1, 0],
            halos.at[1, south_side],
            send_sem.at[2],
            recv_sem.at[2 + south_side],
            south,
        ),
        remote(
            edges.at[1, 1],
            halos.at[1, north_side],
            send_sem.at[3],
            recv_sem.at[2 + north_side],
            north,
        ),
    ]
    def entered(first_send=None):
        with jax.named_scope("barrier"):
            pl.semaphore_wait(barrier, peers)

        if first_send is not None:
            first_send()

        @pl.when(answers)
        def _():
            pl.semaphore_signal(entry_sem, inc=1, device_id=north, device_id_type=MESH)

        @pl.when(is_tail)
        def _():
            tail_copy.start()

        @pl.when(is_half)
        def _():
            tail_0_copy.start()

        for copy in near[:2]:
            copy.start()

        @pl.when(is_root)
        def _():
            for copy in head_copies[3:]:
                copy.start()
            head_0_copy.start()

    def then_send():
        @pl.when(is_root)
        def _():
            for copy in head_copies[:3]:
                copy.start()

        near[3].start()

        @pl.when(jnp.logical_not(asks))
        def _():
            near[2].start()

    @pl.when(jnp.logical_not(is_early | is_mid))
    def _():
        entered()

    with jax.named_scope("turn_m"):
        turn_in(1, (0, 1, 2, 3))

    loads[4].wait()
    loads[5].wait()
    spread = jnp.concatenate([mix[...]] * 4, axis=1)
    row_at = lax.broadcasted_iota(jnp.int32, (LANES, LANES), 0)
    lane_at = lax.broadcasted_iota(jnp.int32, (LANES, LANES), 1)
    spread = jnp.where(row_at // 32 == lane_at // 32, spread, 0.0)
    spread = spread + jnp.where(row_at == lane_at, 0.2, 0.0)
    high, low = two_parts(spread.T)
    for row in (0, LANES):
        weights[row : row + LANES, 0:LANES] = high
        weights[row : row + LANES, LANES:] = low

    def one_way(there, back, courant, items, rows, chunk):
        def src(item, w, at, size):
            return there[item, w, pl.ds(at, size), :]

        def dst(item, w, at, size, value):
            back[item, w, pl.ds(at, size), :] = value

        advance(src, dst, courant, weights, items, rows, chunk)

    def two_steps(there, back, courant, items, rows, chunk):
        one_way(there, back, courant, items, rows, chunk)
        one_way(back, there, courant, items, rows, chunk)

    def interior(f):
        items = [4 * f + r for r in range(4)]

        def courant(ch, at, size):
            return first[ch, 3, pl.ds(OFF + at, size), :]

        def step(t, carry):
            two_steps(state, other_state, courant, items, CELLS, 16)
            return carry

        lax.fori_loop(0, SUB // 2, step, 0)

    def arrived(f, side):
        pltpu.make_async_copy(
            halos.at[f, side], halos.at[f, side], recv_sem.at[2 * f + side]
        ).wait()

    def strip_steps(count):
        def step(t, carry):
            two_steps(
                strips,
                other_strips,
                lambda n, at, size: scour[n, pl.ds(at, size), :],
                list(range(count)),
                WIN,
                16,
            )
            return carry

        lax.fori_loop(0, SUB // 2, step, 0)

    def fill(n, ch, start):
        for w in range(3):
            strips[n, w, OFF : OFF + WIN, :] = first[ch, w, pl.ds(start, WIN), :]
        scour[n, :, :] = first[ch, 3, pl.ds(start, WIN), :]

    left_row, right_row = OFF - SUB, OFF + CELLS
    left_start, right_start = OFF - SUB, OFF + CELLS + SUB - WIN
    near_columns = me * GLON_DEV - 1 + lax.broadcasted_iota(jnp.int32, (8, CELLS), 0)
    column = lax.broadcasted_iota(jnp.int32, (CELLS, LANES), 0)
    scale = GLON_DEV / (3.0 * CELLS)
    back_copy = remote(part.at[4], part_in.at[1], send_sem.at[4], recv_sem.at[5], west)
    on_copy = remote(part.at[5], part_in.at[0], send_sem.at[5], recv_sem.at[4], east)
    is_last = me == lon_count - 1

    def merid_end():
        with jax.named_scope("merid_wait"):
            arrived(1, 0)
            arrived(1, 1)
        for side, turned, row in ((0, at_south, left_row), (1, at_north, right_row)):
            for r in range(4):
                for p in range(4):
                    plain = halos[1, side, r, 4 * p : 4 * p + 4, :]
                    q = p if p == 3 else 2 - p
                    mirrored = jnp.concatenate(
                        [halos[1, side, r, 4 * q + 3 - j : 4 * q + 4 - j, :] for j in range(SUB)],
                        axis=0,
                    )
                    if p == 3:
                        mirrored = -mirrored
                    first[4 + r, p, row : row + SUB, :] = jnp.where(turned, mirrored, plain)
        for r in range(4):
            fill(r, 4 + r, left_start)
            fill(4 + r, 4 + r, right_start)
        with jax.named_scope("merid_strips"):
            strip_steps(8)
        for r in range(4):
            for w in range(3):
                kept = strips[r, w, OFF + 4 : OFF + 8, :]
                state[4 + r, w, OFF : OFF + SUB, :] = kept
                kept = strips[4 + r, w, OFF + 8 : OFF + 12, :]
                state[4 + r, w, OFF + CELLS - SUB : OFF + CELLS, :] = kept
        for r in range(4):
            for w in range(3):
                out_m[pl.ds(w * 4 + r, LANES, stride=12), :] = state[
                    4 + r, w, OFF : OFF + CELLS, :
                ].T

    def shares(r, change):
        high, low = two_parts(change * scale)
        mine = (jnp.broadcast_to(owner[r : r + 1, :], (8, CELLS)) == near_columns).astype(BF16)
        return jnp.dot(
            jnp.concatenate([mine, mine], axis=1),
            jnp.concatenate([high, low], axis=0),
            preferred_element_type=F32,
        )

    def right_strips(at):
        for r in range(4):
            for p in range(4):
                first[r, p, right_row : right_row + SUB, :] = halos[0, 1, r, 4 * p : 4 * p + 4, :]
        for r in range(4):
            fill(at + r, r, right_start)

    def right_kept(at):
        for r in range(4):
            for w in range(3):
                kept = strips[at + r, w, OFF + 8 : OFF + 12, :]
                state[r, w, OFF + CELLS - SUB : OFF + CELLS, :] = kept

    passing = {relay: copies for relay, copies in passed_on.items() if copies}
    is_relay = functools.reduce(jnp.logical_or, [me == relay for relay in passing])

    def heads_arrived():
        pltpu.make_async_copy(heads.at[2:4], heads.at[2:4], recv_sem.at[8]).wait()

    def pass_on():
        with jax.named_scope("pass_on"):
            for relay, copies in passing.items():

                @pl.when(me == relay)
                def _(copies=copies):
                    heads_arrived()
                    for copy in copies:
                        copy.start()

    def left_kept(at):
        for r in range(4):
            for w in range(3):
                kept = strips[at + r, w, OFF + 4 : OFF + 8, :]
                state[r, w, OFF : OFF + SUB, :] = kept

    def early_part():
        arrived(0, 1)
        with jax.named_scope("early_part"):
            right_strips(0)
            strip_steps(4)
            right_kept(0)
            for r in range(4):
                change = None
                for w in range(3):
                    value = (
                        state[r, w, OFF : OFF + CELLS, :] - first[r, w, OFF : OFF + CELLS, :]
                    )
                    change = value if change is None else change + value
                change = jnp.where(column >= SUB, change, 0.0)
                part[5, r : r + 1, :] = shares(r, change)[5:6]
            on_copy.start()

    def zonal_end(first_wait=True):
        if first_wait:
            with jax.named_scope("right_wait"):
                arrived(0, 1)

        with jax.named_scope("left_wait"):
            arrived(0, 0)
        for r in range(4):
            for p in range(4):
                first[r, p, left_row : left_row + SUB, :] = halos[0, 0, r, 4 * p : 4 * p + 4, :]

        def edge_strips():
            right_strips(0)
            for r in range(4):
                fill(4 + r, r, left_start)

        def edges_kept():
            right_kept(0)
            left_kept(4)

        def far_arrived():
            with jax.named_scope("far_wait"):

                @pl.when(jnp.logical_not(is_relay))
                def _():
                    heads_arrived()

                @pl.when(is_half)
                def _():
                    pltpu.make_async_copy(heads.at[0], heads.at[0], recv_sem.at[9]).wait()

        def far_strips(at):
            for n, r in enumerate(FAR):
                fill(at + n, r, ends[r])
                for w in range(3):
                    strips[at + n, w, OFF + 8 : OFF + 12, :] = heads[r, 4 * w : 4 * w + 4, :]
                scour[at + n, 8:12, :] = heads[r, 12:16, :]

        def far_kept(at):
            for n in range(len(FAR)):
                for w in range(3):
                    back[n, w, PBASE : PBASE + WIN, :] = strips[at + n, w, OFF : OFF + WIN, :]

        def base_parts():
            for r in range(4):
                change = None
                for w in range(3):
                    value = (
                        state[r, w, OFF : OFF + CELLS, :] - first[r, w, OFF : OFF + CELLS, :]
                    )
                    change = value if change is None else change + value
                if r in FAR:
                    change = jnp.where(column < ends[r] - SUB, change, 0.0)
                    owned = owner[r : r + 1, :].astype(F32)
                    owners[FAR.index(r), OFF : OFF + CELLS, :] = jnp.broadcast_to(
                        owned, (LANES, CELLS)
                    ).T
                part[r, :, :] = shares(r, change)

        in_one = me == half_turn - 1

        @pl.when(in_one)
        def _():
            edge_strips()
            far_arrived()
            far_strips(8)
            with jax.named_scope("zonal_strips"):
                strip_steps(11)
            edges_kept()
            far_kept(8)

        @pl.when(jnp.logical_not(in_one | is_root))
        def _():
            edge_strips()
            with jax.named_scope("zonal_strips"):
                strip_steps(8)
            edges_kept()

        @pl.when(jnp.logical_not(is_root))
        def _():
            base_parts()

        @pl.when(is_tail & jnp.logical_not(in_one))
        def _():
            far_arrived()
            far_strips(0)
            with jax.named_scope("far_strips"):
                strip_steps(3)
            far_kept(0)

        @pl.when(is_root)
        def _():
            with jax.named_scope("far_wait"):
                for n in range(len(tail_devs)):
                    pltpu.make_async_copy(gathered.at[n], gathered.at[n], far_recv.at[n]).wait()
                pltpu.make_async_copy(gathered_0, gathered_0, recv_sem.at[7]).wait()
            for r in FAR:
                if r == 0:
                    tail_cells = gathered_0[...]
                else:
                    tail_cells = gathered[0, r - 2]
                    for n in range(1, len(tail_devs)):
                        tail_cells = tail_cells + gathered[n, r - 2]
                for p in range(4):
                    first[r, p, left_row : left_row + SUB, :] = tail_cells[4 * p : 4 * p + 4]
            for r in range(4):
                fill(r, r, left_start)
            with jax.named_scope("far_strips"):
                strip_steps(4)
            left_kept(0)
            base_parts()

        @pl.when(is_tail)
        def _():
            row = lax.broadcasted_iota(jnp.int32, (8, LANES), 0)
            for n, r in enumerate(FAR):
                cell = ends[r] - 8 + row
                valid = (row >= SUB) & (cell >= 0) & (cell < CELLS)
                change = None
                for w in range(3):
                    value = back[n, w, PBASE : PBASE + 8, :] - first[r, w, pl.ds(ends[r], 8), :]
                    change = value if change is None else change + value
                change = jnp.where(valid, change * scale, 0.0)
                owned = owners[n, pl.ds(ends[r], 8), :]
                sums = [
                    jnp.sum(
                        jnp.where(owned == (me * GLON_DEV - 1 + g).astype(F32), change, 0.0),
                        axis=0,
                        keepdims=True,
                    )
                    for g in range(GLON_DEV + 2)
                ]
                sums.append(jnp.zeros((2, LANES), F32))
                part[r, :, :] = part[r, :, :] + jnp.concatenate(sums, axis=0)

        @pl.when(jnp.logical_not(is_root))
        def _():
            for r in range(4):
                part[4, r : r + 1, :] = part[r, 0:1, :]
            back_copy.start()

        @pl.when(jnp.logical_not(is_root | is_last))
        def _():
            for r in range(4):
                part[5, r : r + 1, :] = part[r, 5:6, :]
            on_copy.start()

        for n, r in enumerate(FAR):
            for w in range(3):
                value = state[r, w, OFF : OFF + CELLS, :]
                before = first[r, w, OFF : OFF + CELLS, :]
                strip = back[n, w, pl.ds(PBASE + 8 - ends[r], CELLS), :]
                value = jnp.where(column >= ends[r] - SUB, strip, value)
                state[r, w, OFF : OFF + CELLS, :] = jnp.where(column < ends[r], value, before)

    @pl.when(jnp.logical_not(is_early | is_mid))
    def _():
        then_send()

    @pl.when(is_late)
    def _():
        with jax.named_scope("interior_z"):
            interior(0)
        pass_on()

        @pl.when(asks)
        def _():
            with jax.named_scope("answer_wait"):
                pl.semaphore_wait(entry_sem, 1)
            near[2].start()

        zonal_end()
        with jax.named_scope("interior_m"):
            interior(1)
        merid_end()

    @pl.when(jnp.logical_not(is_late))
    def _():
        with jax.named_scope("interior_m"):
            interior(1)

        @pl.when(is_mid | is_early)
        def _():
            entered(then_send)

        with jax.named_scope("interior_z"):
            interior(0)

        @pl.when(is_root)
        def _():
            early_part()

        @pl.when(is_early | is_mid)
        def _():
            pass_on()

        @pl.when(jnp.logical_not(is_root))
        def _():
            with jax.named_scope("right_wait"):
                arrived(0, 1)

        @pl.when(jnp.logical_not(zonal_first))
        def _():
            merid_end()

        @pl.when(jnp.logical_not(is_early | is_mid))
        def _():
            pass_on()

        zonal_end(False)

        @pl.when(zonal_first)
        def _():
            merid_end()

    for r in range(4):
        for w in range(3):
            out_z[pl.ds(w * 4 + r, LANES, stride=12), :] = state[r, w, OFF : OFF + CELLS, :].T

    with jax.named_scope("part_wait"):

        @pl.when(is_root)
        def _():
            part_in[0, :, :] = jnp.zeros((8, LANES), F32)

        @pl.when(is_last)
        def _():
            part_in[1, :, :] = jnp.zeros((8, LANES), F32)

        @pl.when(jnp.logical_not(is_last))
        def _():
            back_copy.wait_recv()

        @pl.when(jnp.logical_not(is_root))
        def _():
            on_copy.wait_recv()

    for r in range(4):
        for g in range(GLON_DEV):
            value = part[r, g + 1 : g + 2, :]
            if g == 0:
                value = value + part_in[0, r : r + 1, :]
            if g == GLON_DEV - 1:
                value = value + part_in[1, r : r + 1, :]
            out_c[4 * g + r : 4 * g + r + 1, :] = value

    for copy in near:
        copy.wait_send()

    @pl.when(jnp.logical_not(is_root))
    def _():
        back_copy.wait_send()

    @pl.when(jnp.logical_not(is_last))
    def _():
        on_copy.wait_send()

    @pl.when(is_tail)
    def _():
        tail_copy.wait_send()

    @pl.when(is_half)
    def _():
        tail_0_copy.wait_send()

    for relay, copies in passing.items():

        @pl.when(me == relay)
        def _(copies=copies):
            for copy in copies:
                copy.wait_send()

    @pl.when(is_root)
    def _():
        head_0_copy.wait_send()
        for copy in head_copies:
            copy.wait_send()


def write_out(z, m, c, out_z, out_m, out_c, sem):
    copies = [
        pltpu.make_async_copy(src, dst, sem.at[n])
        for n, (src, dst) in enumerate(((z, out_z), (m, out_m), (c, out_c)))
    ]
    for copy in copies:
        copy.start()
    for copy in copies:
        copy.wait()


def shards(
    counts, zonal_state, zonal_courant, zonal_length, zonal_owner, merid_state, merid_courant, mixing
):
    tail_count = counts[0] - (counts[0] // 4 - 1)
    relays = relays_of(counts[0])
    hbm = pl.BlockSpec(memory_space=pltpu.HBM)
    vmem = pl.BlockSpec(memory_space=pltpu.VMEM)
    flat_shape = (LANES * 12, CELLS)

    def in_hbm(array, shape):
        return pltpu.with_memory_space_constraint(array.reshape(shape), pltpu.HBM)

    out_z, out_m, out_c = pl.pallas_call(
        functools.partial(kernel, counts),
        out_shape=(
            pltpu.VMEM(flat_shape, F32),
            pltpu.VMEM(flat_shape, F32),
            pltpu.VMEM((4 * GLON_DEV, LANES), F32),
        ),
        in_specs=[hbm, hbm, hbm, hbm, hbm, hbm, hbm],
        out_specs=(vmem, vmem, vmem),
        scratch_shapes=[
            pltpu.VMEM((2, *flat_shape), F32),
            pltpu.VMEM((2, LANES, CELLS), F32),
            pltpu.VMEM((4, CELLS), jnp.int32),
            pltpu.VMEM((LANES, 32), F32),
            pltpu.SMEM((4,), jnp.int32),
            pltpu.VMEM((8, 4, ROWS, LANES), F32),
            pltpu.VMEM((8, 3, ROWS, LANES), F32),
            pltpu.VMEM((8, 3, ROWS, LANES), F32),
            pltpu.VMEM((2 * LANES, 2 * LANES), BF16),
            pltpu.VMEM((12, 3, SROWS, LANES), F32),
            pltpu.VMEM((12, 3, SROWS, LANES), F32),
            pltpu.VMEM((12, WIN, LANES), F32),
            pltpu.VMEM((3, 3, PROWS, LANES), F32),
            pltpu.VMEM((3, ROWS, LANES), F32),
            pltpu.VMEM((2, 2, 4, 16, LANES), F32),
            pltpu.VMEM((2, 2, 4, 16, LANES), F32),
            pltpu.VMEM((4, 16, LANES), F32),
            pltpu.VMEM((tail_count, 2, 16, LANES), F32),
            pltpu.VMEM((16, LANES), F32),
            pltpu.VMEM((4, 16, LANES), F32),
            pltpu.VMEM((6, 8, LANES), F32),
            pltpu.VMEM((2, 8, LANES), F32),
            pltpu.SemaphoreType.DMA((4, 2)),
            pltpu.SemaphoreType.DMA((6,)),
            pltpu.SemaphoreType.DMA((10,)),
            pltpu.SemaphoreType.DMA((2 + max(map(len, (relays, *relays.values()))),)),
            pltpu.SemaphoreType.DMA((tail_count,)),
            pltpu.SemaphoreType.REGULAR,
        ],
        compiler_params=pltpu.CompilerParams(
            collective_id=0, has_side_effects=True, vmem_limit_bytes=32 * 1024 * 1024
        ),
    )(
        in_hbm(zonal_length, (4,)),
        in_hbm(zonal_state, flat_shape),
        in_hbm(zonal_courant, (LANES, CELLS)),
        in_hbm(zonal_owner, (4, CELLS)),
        in_hbm(merid_state, flat_shape),
        in_hbm(merid_courant, (LANES, CELLS)),
        in_hbm(mixing, (LANES, 32)),
    )
    out_z, out_m, out_c = pl.pallas_call(
        write_out,
        out_shape=(
            pltpu.HBM(flat_shape, F32),
            pltpu.HBM(flat_shape, F32),
            pltpu.HBM((4 * GLON_DEV, LANES), F32),
        ),
        in_specs=[vmem, vmem, vmem],
        out_specs=(hbm, hbm, hbm),
        scratch_shapes=[pltpu.SemaphoreType.DMA((3,))],
        compiler_params=pltpu.CompilerParams(vmem_limit_bytes=1024 * 1024),
    )(out_z, out_m, out_c)
    return (
        out_z.reshape(zonal_state.shape),
        out_m.reshape(merid_state.shape),
        out_c.reshape(GLON_DEV, 4, LANES),
    )


def solution(mesh):
    counts = (mesh.shape["lon"], mesh.shape["lat"])
    return jax.shard_map(
        functools.partial(shards, counts),
        mesh=mesh,
        in_specs=(
            P(None, None, None, "lat", "lon"),
            P(None, "lat", "lon"),
            P("lat"),
            P("lat", "lon"),
            P(None, None, None, "lon", "lat"),
            P(None, "lon", "lat"),
            P(),
        ),
        out_specs=(
            P(None, None, None, "lat", "lon"),
            P(None, None, None, "lon", "lat"),
            P("lon", "lat", None),
        ),
        check_vma=False,
    )
```

```python
import functools

import jax
import jax.numpy as jnp
from jax import lax
from jax.experimental import pallas as pl
from jax.experimental.pallas import tpu as pltpu
from jax.sharding import PartitionSpec as P

SUB = 4
OFF = 8
CELLS = 128
LANES = 128
ROWS = 152
WIN = 16
SROWS = 32
PROWS = 272
PBASE = 136
GLON_DEV = 4
FAR = (0, 2, 3)
MESH = pl.DeviceIdType.MESH
F32 = jnp.float32
BF16 = jnp.bfloat16


def two_parts(value):
    high = value.astype(BF16)
    low = (value - high.astype(F32)).astype(BF16)
    return high, low


def advance(src, dst, courant, weights, items, rows, chunk):
    group = max(1, CELLS // rows)
    for first_item in range(0, len(items), group):
        some = items[first_item : first_item + group]
        parts = [
            jnp.concatenate(two_parts(src(item, w, OFF, rows)), axis=1)
            for item in some
            for w in range(3)
        ]
        product = jnp.dot(
            jnp.concatenate(parts, axis=0), weights[...], preferred_element_type=F32
        )
        for n, item in enumerate(some):
            for at in range(0, rows, chunk):
                half = 0.5 * courant(item, at, chunk)
                ahead_share, behind_share = 0.3 - half, 0.3 + half
                here = [src(item, w, OFF + at, chunk) for w in range(3)]
                for w, (one, other) in enumerate(((0, 1), (0, 2), (1, 2))):
                    spot = (n * 3 + w) * rows + at
                    mixed = (
                        product[spot : spot + chunk, 0:LANES] + product[spot : spot + chunk, LANES:]
                    )
                    along = ahead_share * src(item, w, OFF + at + 1, chunk) + behind_share * src(
                        item, w, OFF + at - 1, chunk
                    )
                    dst(item, w, OFF + at, chunk, mixed + along + 0.1 * (here[one] + here[other]))


def relays_of(lon_count):
    tail_from, half_turn = lon_count // 4 - 1, lon_count // 2
    first_ones = (half_turn + tail_from, tail_from, half_turn - 1, lon_count - 1, half_turn)
    relays = {dev: [] for dev in first_ones}
    for first, last in ((tail_from, half_turn - 1), (half_turn + tail_from, lon_count - 1)):
        for dev in range(first + 1, last):
            relays[first if dev <= first + 2 else last].append(dev)
    for dev in range(half_turn + 1, half_turn + tail_from):
        relays[dev] = []
    return relays


def kernel(
    counts,
    zlen_ref,
    zs,
    zc,
    owner_ref,
    ms,
    mc,
    mix_ref,
    out_z,
    out_m,
    out_c,
    raw,
    rawc,
    owner,
    mix,
    zlen,
    first,
    state,
    other_state,
    weights,
    strips,
    other_strips,
    scour,
    back,
    owners,
    edges,
    halos,
    tails,
    gathered,
    gathered_0,
    heads,
    part,
    part_in,
    load_sem,
    send_sem,
    recv_sem,
    far_send,
    far_recv,
    entry_sem,
):
    lon_count, lat_count = counts
    half_turn = lon_count // 2
    tail_from = lon_count // 4 - 1
    tail_devs = list(range(tail_from, lon_count))
    relays = relays_of(lon_count)
    me, lat = lax.axis_index("lon"), lax.axis_index("lat")
    left = lax.rem(me + lon_count - 1, lon_count)
    right = lax.rem(me + 1, lon_count)
    across = lax.rem(me + half_turn, lon_count)
    at_south, at_north = lat == 0, lat == lat_count - 1
    south = {"lon": jnp.where(at_south, across, me), "lat": jnp.where(at_south, lat, lat - 1)}
    north = {"lon": jnp.where(at_north, across, me), "lat": jnp.where(at_north, lat, lat + 1)}
    west, east = {"lon": left, "lat": lat}, {"lon": right, "lat": lat}
    root = {"lon": 0 * me, "lat": lat}
    is_root, is_tail, is_half = me == 0, me >= tail_from, me == half_turn

    loads = []
    for f, (s_ref, c_ref) in enumerate(((zs, zc), (ms, mc))):
        loads.append(pltpu.make_async_copy(s_ref, raw.at[f], load_sem.at[f, 0]))
        loads.append(pltpu.make_async_copy(c_ref, rawc.at[f], load_sem.at[f, 1]))
    loads.append(pltpu.make_async_copy(mix_ref, mix, load_sem.at[2, 0]))
    loads.append(pltpu.make_async_copy(owner_ref, owner, load_sem.at[2, 1]))
    loads.append(pltpu.make_async_copy(zlen_ref, zlen, load_sem.at[3, 0]))
    for load in loads:
        load.start()

    place = lax.rem(me, half_turn)
    is_late, is_early = place >= half_turn // 2, place == 0
    in_middle = (lat == lat_count // 2 - 1) | (lat == lat_count // 2)
    is_mid = (place == tail_from) | (in_middle & jnp.logical_not(is_late | is_early))
    answers = is_late & (lat == lat_count // 2 - 1)
    asks = is_late & (lat == lat_count // 2)

    barrier = pltpu.get_barrier_semaphore()
    for peer in (west, east, south):
        pl.semaphore_signal(barrier, inc=1, device_id=peer, device_id_type=MESH)

    @pl.when(jnp.logical_not(answers))
    def _():
        pl.semaphore_signal(barrier, inc=1, device_id=north, device_id_type=MESH)

    def sector(dev):
        return {"lon": 0 * me + dev, "lat": lat}

    child_count = 0 * me
    for relay, children in relays.items():
        child_count = child_count + jnp.where(me == relay, len(children), 0)

        @pl.when(me == relay)
        def _():
            pl.semaphore_signal(barrier, inc=1, device_id=root, device_id_type=MESH)

        if children:

            @pl.when((me >= children[0]) & (me <= children[-1]))
            def _(relay=relay):
                pl.semaphore_signal(
                    barrier, inc=1, device_id=sector(relay), device_id_type=MESH
                )

    zonal_first = jnp.logical_not(is_root)
    peers = 4 - jnp.where(asks, 1, 0) + jnp.where(is_tail, 1, 0) + child_count + jnp.where(is_root, len(relays), 0)

    @pl.when(is_root)
    def _():
        for dev in tail_devs:
            pl.semaphore_signal(
                barrier, inc=1, device_id={"lon": 0 * me + dev, "lat": lat}, device_id_type=MESH
            )

    def turn_in(f, channels):
        if channels[0] != 1:
            loads[2 * f].wait()
            loads[2 * f + 1].wait()
        for r in channels:
            for w in range(3):
                turned = raw[f, pl.ds(w * 4 + r, LANES, stride=12), :].T
                first[4 * f + r, w, OFF : OFF + CELLS, :] = turned
                state[4 * f + r, w, OFF : OFF + CELLS, :] = turned
            c_now = rawc[f, pl.ds(r, 32, stride=4), :]
            first[4 * f + r, 3, OFF : OFF + CELLS, :] = jnp.concatenate([c_now] * 4, axis=0).T
        for r in channels:
            for p in range(4):
                edges[f, 0, r, 4 * p : 4 * p + 4, :] = first[4 * f + r, p, OFF : OFF + SUB, :]
                edges[f, 1, r, 4 * p : 4 * p + 4, :] = first[
                    4 * f + r, p, OFF + CELLS - SUB : OFF + CELLS, :
                ]

    with jax.named_scope("turn_z"):
        turn_in(0, (2, 3, 0))
        loads[6].wait()
        ends = [jnp.clip(zlen[r] - me * CELLS, 0, CELLS + SUB) for r in range(4)]
        quarter = lax.broadcasted_iota(jnp.int32, (8, LANES), 0)
        for r in FAR:
            cell = ends[r] - SUB + quarter
            own = (cell >= 0) & (cell < CELLS)
            for p in range(4):
                found = jnp.where(own, first[r, p, pl.ds(OFF + ends[r] - SUB, 8), :], 0.0)
                tails[r, 4 * p : 4 * p + 4, :] = found[0:SUB]
        turn_in(0, (1,))

    def remote(src, dst, s_sem, r_sem, peer):
        return pltpu.make_async_remote_copy(
            src_ref=src,
            dst_ref=dst,
            send_sem=s_sem,
            recv_sem=r_sem,
            device_id=peer,
            device_id_type=MESH,
        )

    slot = jnp.maximum(me - tail_from, 0)
    tail_copy = remote(
        tails.at[2:4], gathered.at[slot], far_send.at[0], far_recv.at[slot], root
    )
    tail_0_copy = remote(
        tails.at[0], gathered_0, far_send.at[1], recv_sem.at[7], root
    )
    head_copies = [
        remote(
            edges.at[0, 0, 2:4], heads.at[2:4], far_send.at[2 + n], recv_sem.at[8], sector(relay)
        )
        for n, relay in enumerate(relays)
    ]
    head_0_copy = remote(
        edges.at[0, 0, 0], heads.at[0], far_send.at[1], recv_sem.at[9], sector(half_turn)
    )
    passed_on = {
        relay: [
            remote(heads.at[2:4], heads.at[2:4], far_send.at[2 + n], recv_sem.at[8], sector(dev))
            for n, dev in enumerate(children)
        ]
        for relay, children in relays.items()
    }

    south_side, north_side = jnp.where(at_south, 0, 1), jnp.where(at_north, 1, 0)
    near = [
        remote(edges.at[0, 0], halos.at[0, 1], send_sem.at[0], recv_sem.at[1], west),
        remote(edges.at[0, 1], halos.at[0, 0], send_sem.at[1], recv_sem.at[0], east),
        remote(
            edges.at[1, 0],
            halos.at[1, south_side],
            send_sem.at[2],
            recv_sem.at[2 + south_side],
            south,
        ),
        remote(
            edges.at[1, 1],
            halos.at[1, north_side],
            send_sem.at[3],
            recv_sem.at[2 + north_side],
            north,
        ),
    ]
    def entered(first_send=None):
        with jax.named_scope("barrier"):
            pl.semaphore_wait(barrier, peers)

        if first_send is not None:
            first_send()

        @pl.when(answers)
        def _():
            pl.semaphore_signal(entry_sem, inc=1, device_id=north, device_id_type=MESH)

        @pl.when(is_tail)
        def _():
            tail_copy.start()

        @pl.when(is_half)
        def _():
            tail_0_copy.start()

        for copy in near[:2]:
            copy.start()

        @pl.when(is_root)
        def _():
            for copy in head_copies[3:]:
                copy.start()
            head_0_copy.start()

    def then_send():
        @pl.when(is_root)
        def _():
            for copy in head_copies[:3]:
                copy.start()

        near[3].start()

        @pl.when(jnp.logical_not(asks))
        def _():
            near[2].start()

    @pl.when(jnp.logical_not(is_early | is_mid))
    def _():
        entered()

    with jax.named_scope("turn_m"):
        turn_in(1, (0, 1, 2, 3))

    loads[4].wait()
    loads[5].wait()
    spread = jnp.concatenate([mix[...]] * 4, axis=1)
    row_at = lax.broadcasted_iota(jnp.int32, (LANES, LANES), 0)
    lane_at = lax.broadcasted_iota(jnp.int32, (LANES, LANES), 1)
    spread = jnp.where(row_at // 32 == lane_at // 32, spread, 0.0)
    spread = spread + jnp.where(row_at == lane_at, 0.2, 0.0)
    high, low = two_parts(spread.T)
    for row in (0, LANES):
        weights[row : row + LANES, 0:LANES] = high
        weights[row : row + LANES, LANES:] = low

    def one_way(there, back, courant, items, rows, chunk):
        def src(item, w, at, size):
            return there[item, w, pl.ds(at, size), :]

        def dst(item, w, at, size, value):
            back[item, w, pl.ds(at, size), :] = value

        advance(src, dst, courant, weights, items, rows, chunk)

    def two_steps(there, back, courant, items, rows, chunk):
        one_way(there, back, courant, items, rows, chunk)
        one_way(back, there, courant, items, rows, chunk)

    def interior(f):
        items = [4 * f + r for r in range(4)]

        def courant(ch, at, size):
            return first[ch, 3, pl.ds(OFF + at, size), :]

        def step(t, carry):
            two_steps(state, other_state, courant, items, CELLS, 16)
            return carry

        lax.fori_loop(0, SUB // 2, step, 0)

    def arrived(f, side):
        pltpu.make_async_copy(
            halos.at[f, side], halos.at[f, side], recv_sem.at[2 * f + side]
        ).wait()

    def strip_steps(count):
        def step(t, carry):
            two_steps(
                strips,
                other_strips,
                lambda n, at, size: scour[n, pl.ds(at, size), :],
                list(range(count)),
                WIN,
                16,
            )
            return carry

        if count <= 4:
            for t in range(SUB // 2):
                step(t, 0)
        else:
            lax.fori_loop(0, SUB // 2, step, 0)

    def fill(n, ch, start):
        for w in range(3):
            strips[n, w, OFF : OFF + WIN, :] = first[ch, w, pl.ds(start, WIN), :]
        scour[n, :, :] = first[ch, 3, pl.ds(start, WIN), :]

    left_row, right_row = OFF - SUB, OFF + CELLS
    left_start, right_start = OFF - SUB, OFF + CELLS + SUB - WIN
    near_columns = me * GLON_DEV - 1 + lax.broadcasted_iota(jnp.int32, (8, CELLS), 0)
    column = lax.broadcasted_iota(jnp.int32, (CELLS, LANES), 0)
    scale = GLON_DEV / (3.0 * CELLS)
    back_copy = remote(part.at[4], part_in.at[1], send_sem.at[4], recv_sem.at[5], west)
    on_copy = remote(part.at[5], part_in.at[0], send_sem.at[5], recv_sem.at[4], east)
    is_last = me == lon_count - 1

    def merid_end():
        with jax.named_scope("merid_wait"):
            arrived(1, 0)
            arrived(1, 1)
        for side, turned, row in ((0, at_south, left_row), (1, at_north, right_row)):
            for r in range(4):
                for p in range(4):
                    plain = halos[1, side, r, 4 * p : 4 * p + 4, :]
                    q = p if p == 3 else 2 - p
                    mirrored = jnp.concatenate(
                        [halos[1, side, r, 4 * q + 3 - j : 4 * q + 4 - j, :] for j in range(SUB)],
                        axis=0,
                    )
                    if p == 3:
                        mirrored = -mirrored
                    first[4 + r, p, row : row + SUB, :] = jnp.where(turned, mirrored, plain)
        for r in range(4):
            fill(r, 4 + r, left_start)
            fill(4 + r, 4 + r, right_start)
        with jax.named_scope("merid_strips"):
            strip_steps(8)
        for r in range(4):
            for w in range(3):
                kept = strips[r, w, OFF + 4 : OFF + 8, :]
                state[4 + r, w, OFF : OFF + SUB, :] = kept
                kept = strips[4 + r, w, OFF + 8 : OFF + 12, :]
                state[4 + r, w, OFF + CELLS - SUB : OFF + CELLS, :] = kept
        for r in range(4):
            for w in range(3):
                out_m[pl.ds(w * 4 + r, LANES, stride=12), :] = state[
                    4 + r, w, OFF : OFF + CELLS, :
                ].T

    def shares(r, change):
        high, low = two_parts(change * scale)
        mine = (jnp.broadcast_to(owner[r : r + 1, :], (8, CELLS)) == near_columns).astype(BF16)
        return jnp.dot(
            jnp.concatenate([mine, mine], axis=1),
            jnp.concatenate([high, low], axis=0),
            preferred_element_type=F32,
        )

    def right_strips(at):
        for r in range(4):
            for p in range(4):
                first[r, p, right_row : right_row + SUB, :] = halos[0, 1, r, 4 * p : 4 * p + 4, :]
        for r in range(4):
            fill(at + r, r, right_start)

    def right_kept(at):
        for r in range(4):
            for w in range(3):
                kept = strips[at + r, w, OFF + 8 : OFF + 12, :]
                state[r, w, OFF + CELLS - SUB : OFF + CELLS, :] = kept

    passing = {relay: copies for relay, copies in passed_on.items() if copies}
    is_relay = functools.reduce(jnp.logical_or, [me == relay for relay in passing])

    def heads_arrived():
        pltpu.make_async_copy(heads.at[2:4], heads.at[2:4], recv_sem.at[8]).wait()

    def pass_on():
        with jax.named_scope("pass_on"):
            for relay, copies in passing.items():

                @pl.when(me == relay)
                def _(copies=copies):
                    heads_arrived()
                    for copy in copies:
                        copy.start()

    def left_kept(at):
        for r in range(4):
            for w in range(3):
                kept = strips[at + r, w, OFF + 4 : OFF + 8, :]
                state[r, w, OFF : OFF + SUB, :] = kept

    def early_part():
        arrived(0, 1)
        with jax.named_scope("early_part"):
            right_strips(0)
            strip_steps(4)
            right_kept(0)
            for r in range(4):
                change = None
                for w in range(3):
                    value = (
                        state[r, w, OFF : OFF + CELLS, :] - first[r, w, OFF : OFF + CELLS, :]
                    )
                    change = value if change is None else change + value
                change = jnp.where(column >= SUB, change, 0.0)
                part[5, r : r + 1, :] = shares(r, change)[5:6]
            on_copy.start()

    def zonal_end(first_wait=True):
        if first_wait:
            with jax.named_scope("right_wait"):
                arrived(0, 1)

        with jax.named_scope("left_wait"):
            arrived(0, 0)
        for r in range(4):
            for p in range(4):
                first[r, p, left_row : left_row + SUB, :] = halos[0, 0, r, 4 * p : 4 * p + 4, :]

        def edge_strips():
            right_strips(0)
            for r in range(4):
                fill(4 + r, r, left_start)

        def edges_kept():
            right_kept(0)
            left_kept(4)

        def far_arrived():
            with jax.named_scope("far_wait"):

                @pl.when(jnp.logical_not(is_relay))
                def _():
                    heads_arrived()

                @pl.when(is_half)
                def _():
                    pltpu.make_async_copy(heads.at[0], heads.at[0], recv_sem.at[9]).wait()

        def far_strips(at):
            for n, r in enumerate(FAR):
                fill(at + n, r, ends[r])
                for w in range(3):
                    strips[at + n, w, OFF + 8 : OFF + 12, :] = heads[r, 4 * w : 4 * w + 4, :]
                scour[at + n, 8:12, :] = heads[r, 12:16, :]

        def far_kept(at):
            for n in range(len(FAR)):
                for w in range(3):
                    back[n, w, PBASE : PBASE + WIN, :] = strips[at + n, w, OFF : OFF + WIN, :]

        def base_parts():
            for r in range(4):
                change = None
                for w in range(3):
                    value = (
                        state[r, w, OFF : OFF + CELLS, :] - first[r, w, OFF : OFF + CELLS, :]
                    )
                    change = value if change is None else change + value
                if r in FAR:
                    change = jnp.where(column < ends[r] - SUB, change, 0.0)
                    owned = owner[r : r + 1, :].astype(F32)
                    owners[FAR.index(r), OFF : OFF + CELLS, :] = jnp.broadcast_to(
                        owned, (LANES, CELLS)
                    ).T
                part[r, :, :] = shares(r, change)

        in_one = me == half_turn - 1

        @pl.when(in_one)
        def _():
            edge_strips()
            far_arrived()
            far_strips(8)
            with jax.named_scope("zonal_strips"):
                strip_steps(11)
            edges_kept()
            far_kept(8)

        @pl.when(jnp.logical_not(in_one | is_root))
        def _():
            edge_strips()
            with jax.named_scope("zonal_strips"):
                strip_steps(8)
            edges_kept()

        @pl.when(jnp.logical_not(is_root))
        def _():
            base_parts()

        @pl.when(is_tail & jnp.logical_not(in_one))
        def _():
            far_arrived()
            far_strips(0)
            with jax.named_scope("far_strips"):
                strip_steps(3)
            far_kept(0)

        @pl.when(is_root)
        def _():
            with jax.named_scope("far_wait"):
                for n in range(len(tail_devs)):
                    pltpu.make_async_copy(gathered.at[n], gathered.at[n], far_recv.at[n]).wait()
                pltpu.make_async_copy(gathered_0, gathered_0, recv_sem.at[7]).wait()
            for r in FAR:
                if r == 0:
                    tail_cells = gathered_0[...]
                else:
                    tail_cells = gathered[0, r - 2]
                    for n in range(1, len(tail_devs)):
                        tail_cells = tail_cells + gathered[n, r - 2]
                for p in range(4):
                    first[r, p, left_row : left_row + SUB, :] = tail_cells[4 * p : 4 * p + 4]
            for r in range(4):
                fill(r, r, left_start)
            with jax.named_scope("far_strips"):
                strip_steps(4)
            left_kept(0)
            base_parts()

        @pl.when(is_tail)
        def _():
            row = lax.broadcasted_iota(jnp.int32, (8, LANES), 0)
            for n, r in enumerate(FAR):
                cell = ends[r] - 8 + row
                valid = (row >= SUB) & (cell >= 0) & (cell < CELLS)
                change = None
                for w in range(3):
                    value = back[n, w, PBASE : PBASE + 8, :] - first[r, w, pl.ds(ends[r], 8), :]
                    change = value if change is None else change + value
                change = jnp.where(valid, change * scale, 0.0)
                owned = owners[n, pl.ds(ends[r], 8), :]
                sums = [
                    jnp.sum(
                        jnp.where(owned == (me * GLON_DEV - 1 + g).astype(F32), change, 0.0),
                        axis=0,
                        keepdims=True,
                    )
                    for g in range(GLON_DEV + 2)
                ]
                sums.append(jnp.zeros((2, LANES), F32))
                part[r, :, :] = part[r, :, :] + jnp.concatenate(sums, axis=0)

        @pl.when(jnp.logical_not(is_root))
        def _():
            for r in range(4):
                part[4, r : r + 1, :] = part[r, 0:1, :]
            back_copy.start()

        @pl.when(jnp.logical_not(is_root | is_last))
        def _():
            for r in range(4):
                part[5, r : r + 1, :] = part[r, 5:6, :]
            on_copy.start()

        for n, r in enumerate(FAR):
            for w in range(3):
                value = state[r, w, OFF : OFF + CELLS, :]
                before = first[r, w, OFF : OFF + CELLS, :]
                strip = back[n, w, pl.ds(PBASE + 8 - ends[r], CELLS), :]
                value = jnp.where(column >= ends[r] - SUB, strip, value)
                state[r, w, OFF : OFF + CELLS, :] = jnp.where(column < ends[r], value, before)

    @pl.when(jnp.logical_not(is_early | is_mid))
    def _():
        then_send()

    @pl.when(is_late)
    def _():
        with jax.named_scope("interior_z"):
            interior(0)
        pass_on()

        @pl.when(asks)
        def _():
            with jax.named_scope("answer_wait"):
                pl.semaphore_wait(entry_sem, 1)
            near[2].start()

        zonal_end()
        with jax.named_scope("interior_m"):
            interior(1)
        merid_end()

    @pl.when(jnp.logical_not(is_late))
    def _():
        with jax.named_scope("interior_m"):
            interior(1)

        @pl.when(is_mid | is_early)
        def _():
            entered(then_send)

        with jax.named_scope("interior_z"):
            interior(0)

        @pl.when(is_root)
        def _():
            early_part()

        @pl.when(is_early | is_mid)
        def _():
            pass_on()

        @pl.when(jnp.logical_not(is_root))
        def _():
            with jax.named_scope("right_wait"):
                arrived(0, 1)

        @pl.when(jnp.logical_not(zonal_first))
        def _():
            merid_end()

        @pl.when(jnp.logical_not(is_early | is_mid))
        def _():
            pass_on()

        zonal_end(False)

        @pl.when(zonal_first)
        def _():
            merid_end()

    for r in range(4):
        for w in range(3):
            out_z[pl.ds(w * 4 + r, LANES, stride=12), :] = state[r, w, OFF : OFF + CELLS, :].T

    with jax.named_scope("part_wait"):

        @pl.when(is_root)
        def _():
            part_in[0, :, :] = jnp.zeros((8, LANES), F32)

        @pl.when(is_last)
        def _():
            part_in[1, :, :] = jnp.zeros((8, LANES), F32)

        @pl.when(jnp.logical_not(is_last))
        def _():
            back_copy.wait_recv()

        @pl.when(jnp.logical_not(is_root))
        def _():
            on_copy.wait_recv()

    for r in range(4):
        for g in range(GLON_DEV):
            value = part[r, g + 1 : g + 2, :]
            if g == 0:
                value = value + part_in[0, r : r + 1, :]
            if g == GLON_DEV - 1:
                value = value + part_in[1, r : r + 1, :]
            out_c[4 * g + r : 4 * g + r + 1, :] = value

    for copy in near:
        copy.wait_send()

    @pl.when(jnp.logical_not(is_root))
    def _():
        back_copy.wait_send()

    @pl.when(jnp.logical_not(is_last))
    def _():
        on_copy.wait_send()

    @pl.when(is_tail)
    def _():
        tail_copy.wait_send()

    @pl.when(is_half)
    def _():
        tail_0_copy.wait_send()

    for relay, copies in passing.items():

        @pl.when(me == relay)
        def _(copies=copies):
            for copy in copies:
                copy.wait_send()

    @pl.when(is_root)
    def _():
        head_0_copy.wait_send()
        for copy in head_copies:
            copy.wait_send()


def write_out(z, m, c, out_z, out_m, out_c, sem):
    copies = [
        pltpu.make_async_copy(src, dst, sem.at[n])
        for n, (src, dst) in enumerate(((z, out_z), (m, out_m), (c, out_c)))
    ]
    for copy in copies:
        copy.start()
    for copy in copies:
        copy.wait()


def shards(
    counts, zonal_state, zonal_courant, zonal_length, zonal_owner, merid_state, merid_courant, mixing
):
    tail_count = counts[0] - (counts[0] // 4 - 1)
    relays = relays_of(counts[0])
    hbm = pl.BlockSpec(memory_space=pltpu.HBM)
    vmem = pl.BlockSpec(memory_space=pltpu.VMEM)
    flat_shape = (LANES * 12, CELLS)

    def in_hbm(array, shape):
        return pltpu.with_memory_space_constraint(array.reshape(shape), pltpu.HBM)

    out_z, out_m, out_c = pl.pallas_call(
        functools.partial(kernel, counts),
        out_shape=(
            pltpu.VMEM(flat_shape, F32),
            pltpu.VMEM(flat_shape, F32),
            pltpu.VMEM((4 * GLON_DEV, LANES), F32),
        ),
        in_specs=[hbm, hbm, hbm, hbm, hbm, hbm, hbm],
        out_specs=(vmem, vmem, vmem),
        scratch_shapes=[
            pltpu.VMEM((2, *flat_shape), F32),
            pltpu.VMEM((2, LANES, CELLS), F32),
            pltpu.VMEM((4, CELLS), jnp.int32),
            pltpu.VMEM((LANES, 32), F32),
            pltpu.SMEM((4,), jnp.int32),
            pltpu.VMEM((8, 4, ROWS, LANES), F32),
            pltpu.VMEM((8, 3, ROWS, LANES), F32),
            pltpu.VMEM((8, 3, ROWS, LANES), F32),
            pltpu.VMEM((2 * LANES, 2 * LANES), BF16),
            pltpu.VMEM((12, 3, SROWS, LANES), F32),
            pltpu.VMEM((12, 3, SROWS, LANES), F32),
            pltpu.VMEM((12, WIN, LANES), F32),
            pltpu.VMEM((3, 3, PROWS, LANES), F32),
            pltpu.VMEM((3, ROWS, LANES), F32),
            pltpu.VMEM((2, 2, 4, 16, LANES), F32),
            pltpu.VMEM((2, 2, 4, 16, LANES), F32),
            pltpu.VMEM((4, 16, LANES), F32),
            pltpu.VMEM((tail_count, 2, 16, LANES), F32),
            pltpu.VMEM((16, LANES), F32),
            pltpu.VMEM((4, 16, LANES), F32),
            pltpu.VMEM((6, 8, LANES), F32),
            pltpu.VMEM((2, 8, LANES), F32),
            pltpu.SemaphoreType.DMA((4, 2)),
            pltpu.SemaphoreType.DMA((6,)),
            pltpu.SemaphoreType.DMA((10,)),
            pltpu.SemaphoreType.DMA((2 + max(map(len, (relays, *relays.values()))),)),
            pltpu.SemaphoreType.DMA((tail_count,)),
            pltpu.SemaphoreType.REGULAR,
        ],
        compiler_params=pltpu.CompilerParams(
            collective_id=0, has_side_effects=True, vmem_limit_bytes=32 * 1024 * 1024
        ),
    )(
        in_hbm(zonal_length, (4,)),
        in_hbm(zonal_state, flat_shape),
        in_hbm(zonal_courant, (LANES, CELLS)),
        in_hbm(zonal_owner, (4, CELLS)),
        in_hbm(merid_state, flat_shape),
        in_hbm(merid_courant, (LANES, CELLS)),
        in_hbm(mixing, (LANES, 32)),
    )
    out_z, out_m, out_c = pl.pallas_call(
        write_out,
        out_shape=(
            pltpu.HBM(flat_shape, F32),
            pltpu.HBM(flat_shape, F32),
            pltpu.HBM((4 * GLON_DEV, LANES), F32),
        ),
        in_specs=[vmem, vmem, vmem],
        out_specs=(hbm, hbm, hbm),
        scratch_shapes=[pltpu.SemaphoreType.DMA((3,))],
        compiler_params=pltpu.CompilerParams(vmem_limit_bytes=1024 * 1024),
    )(out_z, out_m, out_c)
    return (
        out_z.reshape(zonal_state.shape),
        out_m.reshape(merid_state.shape),
        out_c.reshape(GLON_DEV, 4, LANES),
    )


def solution(mesh):
    counts = (mesh.shape["lon"], mesh.shape["lat"])
    return jax.shard_map(
        functools.partial(shards, counts),
        mesh=mesh,
        in_specs=(
            P(None, None, None, "lat", "lon"),
            P(None, "lat", "lon"),
            P("lat"),
            P("lat", "lon"),
            P(None, None, None, "lon", "lat"),
            P(None, "lon", "lat"),
            P(),
        ),
        out_specs=(
            P(None, None, None, "lat", "lon"),
            P(None, None, None, "lon", "lat"),
            P("lon", "lat", None),
        ),
        check_vma=False,
    )
```
